32 devices in a mesh: dp: 2 (over x), tp: 4 (over z), sp: 4 (over y, core).
Axes of the slice: x: 2, y: 2, z: 4, core: 2. Of those that a mesh axis runs over, the one named last changes fastest.
Arguments:
- hidden: bfloat16 [128, 3072], P('dp'), parts along dimension 0
- positions: int32 [128], P('dp'), parts along dimension 0
- k_cache: bfloat16 [2, 128, 512, 8, 128], P(None, 'dp', 'sp', 'tp'), parts along dimension 1
- v_cache: bfloat16 [2, 128, 512, 8, 128], P(None, 'dp', 'sp', 'tp'), parts along dimension 1
- ln_gain: bfloat16 [2, 2, 3072], replicated
- ln_bias: bfloat16 [2, 2, 3072], replicated
- w_qkv: bfloat16 [2, 3072, 5120], P(None, None, 'tp')
- b_qkv: bfloat16 [2, 5120], P(None, 'tp')
- w_dense: bfloat16 [2, 3072, 3072], P(None, 'tp')
- b_dense: bfloat16 [2, 3072], replicated
- w_up: bfloat16 [2, 3072, 16384], P(None, None, 'tp')
- b_up: bfloat16 [2, 16384], P(None, 'tp')
- w_down: bfloat16 [2, 8192, 3072], P(None, 'tp')
- b_down: bfloat16 [2, 3072], replicated
Outputs:
- output 1: bfloat16 [128, 3072], P('dp'), parts along dimension 0
- output 2: bfloat16 [2, 128, 512, 8, 128], P(None, 'dp', 'sp', 'tp'), parts along dimension 1
- output 3: bfloat16 [2, 128, 512, 8, 128], P(None, 'dp', 'sp', 'tp'), parts along dimension 1
There are 2 independent parts. The reference program is written for one: setup_inputs(seed, part) draws one part's arguments, and reference() takes and returns one part's arrays. A program takes and returns all parts, laid end to end along the dimension named above; an argument that names none is the same for every part.
All inputs are finite; a program needn't handle non-finite values.
Results may differ from the reference program's by a relative error of at most 0.017103.
Values sent between devices are 32-bit elements.
A program may use at most 1 GiB of HBM per device.

```python
import functools
import jax
import jax.numpy as jnp
from jax import lax

NUM_SEQS = 64
SEQ_LEN = 512
D_MODEL = 3072
N_HEADS = 24
KV_HEADS = 8
HEAD_DIM = 128
FF_DIM = 8192
BLOCK_SIZE = 64
LOCAL_BLOCKS = 16
VERT_STRIDE = 8
ROPE_THETA = 1000000.0
GELU_LIMIT = 20.0
NORM_EPS = 0.00001
MASKED = -1e30
GROUP_SIZE = N_HEADS // KV_HEADS
QKV_COLS = KV_HEADS * (GROUP_SIZE + 2) * HEAD_DIM
QK_GAIN = (3.0 * HEAD_DIM ** 0.5) ** 0.5
V_GAIN = 1.5


def normal_draw(key, shape, scale):
    return (jax.random.normal(key, shape, jnp.float32) * scale).astype(jnp.bfloat16)


def setup_inputs(seed: int = 0, part: int = 0) -> dict:
    base = jax.random.key(seed)
    shared = jax.random.split(base, 10)
    local = jax.random.split(jax.random.fold_in(base, part), 4)
    slot_gain = jnp.concatenate([jnp.full((GROUP_SIZE + 1,), QK_GAIN, jnp.float32), jnp.full((1,), V_GAIN, jnp.float32)])
    col_gain = jnp.tile(jnp.repeat(slot_gain, HEAD_DIM), KV_HEADS)
    seq_ids = jnp.arange(NUM_SEQS)
    rand_pos = jax.random.randint(local[1], (NUM_SEQS,), 0, SEQ_LEN)
    positions = jnp.where(seq_ids == 0, SEQ_LEN - 1, jnp.where(seq_ids == 1, SEQ_LEN // 2 + BLOCK_SIZE // 2, rand_pos))
    cache_shape = (2, NUM_SEQS, SEQ_LEN, KV_HEADS, HEAD_DIM)
    return {
        'hidden': normal_draw(local[0], (NUM_SEQS, D_MODEL), 1.0),
        'positions': positions.astype(jnp.int32),
        'k_cache': normal_draw(local[2], cache_shape, QK_GAIN),
        'v_cache': normal_draw(local[3], cache_shape, V_GAIN),
        'ln_gain': jax.random.uniform(shared[0], (2, 2, D_MODEL), jnp.float32, 0.5, 1.5).astype(jnp.bfloat16),
        'ln_bias': normal_draw(shared[1], (2, 2, D_MODEL), 0.3),
        'w_qkv': normal_draw(shared[2], (2, D_MODEL, QKV_COLS), col_gain * D_MODEL ** -0.5),
        'b_qkv': normal_draw(shared[3], (2, QKV_COLS), col_gain * 0.5),
        'w_dense': normal_draw(shared[4], (2, N_HEADS * HEAD_DIM, D_MODEL), (N_HEADS * HEAD_DIM) ** -0.5),
        'b_dense': normal_draw(shared[5], (2, D_MODEL), 0.3),
        'w_up': normal_draw(shared[6], (2, D_MODEL, 2 * FF_DIM), D_MODEL ** -0.5),
        'b_up': normal_draw(shared[7], (2, 2 * FF_DIM), 0.3),
        'w_down': normal_draw(shared[8], (2, FF_DIM, D_MODEL), FF_DIM ** -0.5),
        'b_down': normal_draw(shared[9], (2, D_MODEL), 0.3),
    }


def layer_norm(vec, gain, shift):
    wide_vec = vec.astype(jnp.float32)
    mean_val = jnp.mean(wide_vec, axis=-1, keepdims=True)
    variance = jnp.mean(jnp.square(wide_vec - mean_val), axis=-1, keepdims=True)
    normed = (wide_vec - mean_val) * lax.rsqrt(variance + NORM_EPS)
    return (normed * gain.astype(jnp.float32) + shift.astype(jnp.float32)).astype(jnp.bfloat16)


def rotary(col_pairs, positions):
    half_dim = HEAD_DIM // 2
    inv_freq = ROPE_THETA ** (-jnp.arange(half_dim).astype(jnp.float32) * (2.0 / HEAD_DIM))
    angles = positions.astype(jnp.float32)[:, None] * inv_freq[None, :]
    cos_part = jnp.cos(angles)[:, None, None, :]
    sin_part = jnp.sin(angles)[:, None, None, :]
    first_half = col_pairs[..., :half_dim]
    second_half = col_pairs[..., half_dim:]
    return jnp.concatenate([first_half * cos_part - second_half * sin_part, second_half * cos_part + first_half * sin_part], axis=-1)


def gegelu(up_proj):
    col_pairs = up_proj.reshape(up_proj.shape[0], -1, 2)
    gate_part = jnp.minimum(col_pairs[..., 0], GELU_LIMIT)
    linear_part = jnp.clip(col_pairs[..., 1], -GELU_LIMIT, GELU_LIMIT)
    return gate_part * jax.nn.sigmoid(1.702 * gate_part) * (linear_part + 1.0)


def seq_attention(packed, sparse):
    query_rot, key_rows, value_rows, position = packed
    slot_ids = jnp.arange(SEQ_LEN)
    keep_mask = (slot_ids <= position)[None, None, :]
    if sparse:
        blocks = slot_ids // BLOCK_SIZE
        head_ids = jnp.arange(N_HEADS).reshape(KV_HEADS, GROUP_SIZE)
        near_mask = (position // BLOCK_SIZE - blocks) < LOCAL_BLOCKS
        vertical = (blocks[None, None, :] + head_ids[:, :, None] + 1) % VERT_STRIDE == 0
        keep_mask = keep_mask & (near_mask[None, None, :] | vertical)
    scores = jnp.einsum('kgd,skd->kgs', query_rot.astype(jnp.float32), key_rows.astype(jnp.float32)) / HEAD_DIM
    scores = jnp.where(keep_mask, scores, MASKED)
    peak_score = jnp.max(scores, axis=-1, keepdims=True)
    weights = jnp.where(keep_mask, jnp.exp(scores - peak_score), 0.0)
    mixed_vals = jnp.einsum('kgs,skd->kgd', weights, value_rows.astype(jnp.float32))
    return (mixed_vals / jnp.sum(weights, axis=-1, keepdims=True)).astype(jnp.bfloat16)


def decoder_layer(hidden, positions, k_layer, v_layer, params, sparse):
    gains, shifts, w_qkv, b_qkv, w_dense, b_dense, w_up, b_up, w_down, b_down = params
    normed = layer_norm(hidden, gains[0], shifts[0])
    qkv_proj = jnp.dot(normed, w_qkv, preferred_element_type=jnp.float32) + b_qkv.astype(jnp.float32)
    qkv_proj = qkv_proj.reshape(NUM_SEQS, KV_HEADS, GROUP_SIZE + 2, HEAD_DIM)
    turned = rotary(qkv_proj[:, :, :GROUP_SIZE + 1], positions)
    query_rot = turned[:, :, :GROUP_SIZE].astype(jnp.bfloat16)
    k_new = turned[:, :, GROUP_SIZE].astype(jnp.bfloat16)
    v_new = qkv_proj[:, :, GROUP_SIZE + 1].astype(jnp.bfloat16)
    hit_mask = (jnp.arange(SEQ_LEN)[None, :] == positions[:, None])[:, :, None, None]
    k_layer = jnp.where(hit_mask, k_new[:, None], k_layer)
    v_layer = jnp.where(hit_mask, v_new[:, None], v_layer)
    attn_out = lax.map(functools.partial(seq_attention, sparse=sparse), (query_rot, k_layer, v_layer, positions))
    attn_proj = jnp.dot(attn_out.reshape(NUM_SEQS, N_HEADS * HEAD_DIM), w_dense, preferred_element_type=jnp.float32)
    residual = (hidden.astype(jnp.float32) + attn_proj + b_dense.astype(jnp.float32)).astype(jnp.bfloat16)
    normed_two = layer_norm(residual, gains[1], shifts[1])
    up_proj = jnp.dot(normed_two, w_up, preferred_element_type=jnp.float32) + b_up.astype(jnp.float32)
    gated = gegelu(up_proj).astype(jnp.bfloat16)
    down_proj = jnp.dot(gated, w_down, preferred_element_type=jnp.float32)
    out_hidden = (residual.astype(jnp.float32) + down_proj + b_down.astype(jnp.float32)).astype(jnp.bfloat16)
    return out_hidden, k_layer, v_layer


def reference(hidden, positions, k_cache, v_cache, ln_gain, ln_bias, w_qkv, b_qkv, w_dense, b_dense, w_up, b_up, w_down, b_down):
    k_layers = []
    v_layers = []
    for layer_idx in range(2):
        params = tuple(arr[layer_idx] for arr in (ln_gain, ln_bias, w_qkv, b_qkv, w_dense, b_dense, w_up, b_up, w_down, b_down))
        hidden, k_layer, v_layer = decoder_layer(hidden, positions, k_cache[layer_idx], v_cache[layer_idx], params, layer_idx == 0)
        k_layers.append(k_layer)
        v_layers.append(v_layer)
    return hidden, jnp.stack(k_layers), jnp.stack(v_layers)
```

```python
import functools

import jax
import jax.numpy as jnp
import numpy as np
from jax import lax
from jax.experimental import pallas as pl
from jax.experimental.pallas import tpu as pltpu
from jax.sharding import PartitionSpec as P

MESH = pl.DeviceIdType.MESH
F32 = jnp.float32
BF16 = jnp.bfloat16
BLOCK_SIZE = 64
LOCAL_BLOCKS = 16
VERT_STRIDE = 8
ROPE_THETA = 1000000.0
GELU_LIMIT = 20.0
NORM_EPS = 0.00001
MASKED = -1e30

SEQS = 64
ROWS = 16
OWN = 4
SEQ_LEN = 512
SLOTS = 128
D = 3072
HEAD = 128
KV = 2
GROUP = 3
HEADS = KV * GROUP
QKV = 1280
UP = 4096
FF = 2048
STAT = HEADS * HEAD + HEAD
NCH = 3
CH = D // NCH
GRP = 8
NGRP = SEQS // GRP
VMEM_MAX = 67043328


def rope_tables():
    half = HEAD // 2
    inv = (ROPE_THETA ** (-np.arange(half).astype(np.float32) * np.float32(2.0 / HEAD))).astype(np.float32)
    angle = (np.arange(SEQ_LEN).astype(np.float32)[:, None] * inv[None, :]).astype(np.float64)
    cos, sin = np.cos(angle).astype(np.float32), np.sin(angle).astype(np.float32)
    return np.concatenate([cos, cos], 1), np.concatenate([-sin, sin], 1)


def norm_rows(wide, gain, shift):
    mean = jnp.mean(wide, axis=-1, keepdims=True)
    centred = wide - mean
    var = jnp.mean(centred * centred, axis=-1, keepdims=True)
    return (centred * lax.rsqrt(var + NORM_EPS) * gain + shift).astype(BF16)


def param_row(ref, layer, which=None):
    rows = ref[...] if which is None else ref[layer]
    pick = layer if which is None else which
    return rows.astype(F32)[pick:pick + 1]


def round_bf16(x):
    return x.astype(BF16).astype(F32)


def dot(a, b):
    return jnp.dot(a, b, preferred_element_type=F32)


def turn_columns(ref, rows, cos, sin):
    for c in range(KV):
        for g in range(GROUP + 2):
            cols = slice((c * 5 + g) * HEAD, (c * 5 + g + 1) * HEAD)
            x = ref[rows, cols]
            if g <= GROUP:
                x = x * cos + pltpu.roll(x, HEAD // 2, 1) * sin
            ref[rows, cols] = round_bf16(x)


def attend(group, sparse, pos_ref, q8, kbuf, vbuf, acc8, m8, l8):
    t, s = lax.axis_index("tp"), lax.axis_index("sp")
    row = lax.broadcasted_iota(jnp.int32, (8, 2 * SLOTS), 0)
    col = lax.broadcasted_iota(jnp.int32, (8, 2 * SLOTS), 1)
    slot = s * SLOTS + col // KV
    same = (col % KV) == row // GROUP
    vertical = (slot // BLOCK_SIZE + (t * HEADS + row) + 1) % VERT_STRIDE == 0
    for j in range(GRP):
        b = group * GRP + j
        p = pos_ref[b]
        at = pl.ds(pl.multiple_of(b * 8, 8), 8)
        scores = lax.dot_general(q8[at, :].astype(BF16), kbuf[b], (((1,), (1,)), ((), ())), preferred_element_type=F32)
        scores = scores * (1.0 / HEAD)
        keep = (slot < p) & same
        if sparse:
            near = (p // BLOCK_SIZE - slot // BLOCK_SIZE) < LOCAL_BLOCKS
            keep = keep & (near | vertical)
        scores = jnp.where(keep, scores, MASKED)
        peak = jnp.max(scores, axis=-1, keepdims=True)
        weights = jnp.where(keep, jnp.exp(scores - peak), 0.0)
        total = jnp.sum(weights, axis=-1, keepdims=True)
        acc8[at, :] = dot(weights.astype(BF16), vbuf[b])
        m8[at, :] = jnp.broadcast_to(peak, (8, HEAD))
        l8[at, :] = jnp.broadcast_to(total, (8, HEAD))


def pack_stats(stats, acc8, m8, l8):
    lane = lax.broadcasted_iota(jnp.int32, (SEQS, HEAD), 1)
    tail = jnp.zeros((SEQS, HEAD), F32)
    for h in range(HEADS):
        at = pl.ds(h, SEQS, stride=8)
        stats[:, h * HEAD:(h + 1) * HEAD] = acc8[at, :]
        tail = jnp.where(lane == h, m8[at, :], tail)
        tail = jnp.where(lane == HEADS + h, l8[at, :], tail)
    stats[:, HEADS * HEAD:] = tail


def put_new_rows(group, pos_ref, qkv_ref, kbuf, vbuf):
    s = lax.axis_index("sp")
    row = lax.broadcasted_iota(jnp.int32, (16, HEAD), 0)
    group_rows = pl.ds(pl.multiple_of(group * GRP, GRP), GRP)
    pairs = [[qkv_ref[group_rows, (5 * c + which) * HEAD:(5 * c + which + 1) * HEAD] for c in range(KV)]
             for which in (GROUP, GROUP + 1)]
    for j in range(GRP):
        b = group * GRP + j
        local = pos_ref[b] - s * SLOTS
        inside = jnp.where((local >= 0) & (local < SLOTS), 1, 0)
        local = jnp.clip(local, 0, SLOTS - 1)
        at = pl.ds(pl.multiple_of((local // 8) * 16, 16), 16)
        target = jnp.where(inside == 1, local % 8, 99)
        hit = (row // KV) == target
        for buf, (first, second) in zip((kbuf, vbuf), pairs):
            fresh = jnp.where(row % KV == 0, first[j:j + 1], second[j:j + 1])
            buf[b, at, :] = jnp.where(hit, fresh, buf[b, at, :].astype(F32)).astype(BF16)


def entry_kernel(pos_ref, hidden, gain, shift, b_qkv, cos, sin, w_hbm, kc_hbm, vc_hbm,
                 ko_hbm, vo_hbm, qkv, stats, cos_rows, sin_rows,
                 wbuf, kbuf, vbuf, u_s, q8, acc8, m8, l8, wsem, ksem, vsem, kosem, vosem):
    def w_copy(i):
        return pltpu.make_async_copy(w_hbm.at[0, pl.ds(i * CH, CH)], wbuf.at[pl.ds(i * CH, CH)], wsem.at[i])

    def in_copies(g):
        at = pl.ds(g * GRP, GRP)
        return (pltpu.make_async_copy(kc_hbm.at[0, at], kbuf.at[at], ksem.at[g]),
                pltpu.make_async_copy(vc_hbm.at[0, at], vbuf.at[at], vsem.at[g]))

    def out_copies(g):
        at = pl.ds(g * GRP, GRP)
        return (pltpu.make_async_copy(kbuf.at[at], ko_hbm.at[0, at], kosem.at[g]),
                pltpu.make_async_copy(vbuf.at[at], vo_hbm.at[0, at], vosem.at[g]))

    for i in range(NCH):
        w_copy(i).start()
    for g in range(NGRP):
        for copy in in_copies(g):
            copy.start()

    def pick_row(b, carry):
        p = pos_ref[b]
        cos_rows[pl.ds(b, 1), :] = cos[pl.ds(p, 1), :]
        sin_rows[pl.ds(b, 1), :] = sin[pl.ds(p, 1), :]
        return carry

    lax.fori_loop(0, SEQS, pick_row, 0)
    q8[...] = jnp.zeros_like(q8)
    u_s[...] = norm_rows(hidden[...].astype(F32), param_row(gain, 0, 0), param_row(shift, 0, 0))
    for i in range(NCH):
        w_copy(i).wait()
        piece = dot(u_s[:, i * CH:(i + 1) * CH], wbuf[i * CH:(i + 1) * CH, :])
        qkv[...] = piece + param_row(b_qkv, 0) if i == 0 else qkv[...] + piece
    turn_columns(qkv, slice(None), cos_rows[...], sin_rows[...])
    for h in range(HEADS):
        cols = (h // GROUP * 5 + h % GROUP) * HEAD
        q8[pl.ds(h, SEQS, stride=8), :] = qkv[:, cols:cols + HEAD]

    def one_group(g, carry):
        for copy in in_copies(g):
            copy.wait()
        attend(g, True, pos_ref, q8, kbuf, vbuf, acc8, m8, l8)
        put_new_rows(g, pos_ref, qkv, kbuf, vbuf)
        for copy in out_copies(g):
            copy.start()
        return carry

    lax.fori_loop(0, NGRP, one_group, 0)
    pack_stats(stats, acc8, m8, l8)

    def drain(g, carry):
        for copy in out_copies(g):
            copy.wait()
        return carry

    lax.fori_loop(0, NGRP, drain, 0)


def exit_kernel(pos_ref, qkv, hid, kc_hbm, vc_hbm, ka_hbm, va_hbm, hid_out, ko_hbm, vo_hbm,
                kbuf, vbuf, ksem, vsem, kosem, vosem):
    def in_copies(g):
        at = pl.ds(g * GRP, GRP)
        return (pltpu.make_async_copy(kc_hbm.at[1, at], kbuf.at[at], ksem.at[g]),
                pltpu.make_async_copy(vc_hbm.at[1, at], vbuf.at[at], vsem.at[g]))

    def out_copies(g):
        at = pl.ds(g * GRP, GRP)
        return (pltpu.make_async_copy(kbuf.at[at], ko_hbm.at[1, at], kosem.at[g]),
                pltpu.make_async_copy(vbuf.at[at], vo_hbm.at[1, at], vosem.at[g]))

    for g in range(NGRP):
        for copy in in_copies(g):
            copy.start()
    hid_out[...] = hid[...]

    def one_group(g, carry):
        for copy in in_copies(g):
            copy.wait()
        put_new_rows(g, pos_ref, qkv, kbuf, vbuf)
        for copy in out_copies(g):
            copy.start()
        return carry

    lax.fori_loop(0, NGRP, one_group, 0)

    def drain(g, carry):
        for copy in out_copies(g):
            copy.wait()
        return carry

    lax.fori_loop(0, NGRP, drain, 0)


def main_kernel(pos_ref, stats0, qkv0, cos_rows, sin_rows, hidden, gain, shift, b_qkv, b_dense, b_up, b_down,
                wqkv_hbm, wdense_hbm, wup_hbm, wdown_hbm, kc_hbm, vc_hbm,
                hid, qkv1_out,
                wqkv, wdense, wup, wdown, kbuf, vbuf,
                mix, part, summed, spread, x_own, x_all, o16, u16, h_s, m16, qkv1, stats1, fin, q8, acc8, m8, l8,
                w_sem, kv_sem, mix_send, mix_recv, part_send, part_recv, spread_send, spread_recv,
                q_send, q_recv, fin_send, fin_recv):
    t, s = lax.axis_index("tp"), lax.axis_index("sp")
    sends = []

    def send(src, dst, send_sem, recv_sem, axis, peer):
        copy = pltpu.make_async_remote_copy(src_ref=src, dst_ref=dst, send_sem=send_sem, recv_sem=recv_sem,
                                            device_id={axis: peer}, device_id_type=MESH)
        copy.start()
        sends.append(copy)

    def arrived(dst, send_sem, recv_sem, axis, peer):
        pltpu.make_async_remote_copy(src_ref=dst, dst_ref=dst, send_sem=send_sem, recv_sem=recv_sem,
                                     device_id={axis: peer}, device_id_type=MESH).wait_recv()

    barrier = pltpu.get_barrier_semaphore()
    for axis, me in (("tp", t), ("sp", s)):
        for d in range(1, 4):
            pl.semaphore_signal(barrier, inc=1, device_id={axis: lax.rem(me + d, 4)}, device_id_type=MESH)

    cols = [pl.ds(n * CH, CH) for n in range(NCH)]

    def dense_copy(layer, n):
        return pltpu.make_async_copy(wdense_hbm.at[layer, :, cols[n]], wdense.at[:, cols[n]], w_sem.at[0, n])

    def up_copy(layer, n):
        return pltpu.make_async_copy(wup_hbm.at[layer, cols[n]], wup.at[cols[n]], w_sem.at[1, n])

    def down_copy(layer, n):
        return pltpu.make_async_copy(wdown_hbm.at[layer, :, cols[n]], wdown.at[:, cols[n]], w_sem.at[2, n])

    def qkv_copy(n):
        return pltpu.make_async_copy(wqkv_hbm.at[1, cols[n]], wqkv.at[cols[n]], w_sem.at[3, n])

    k_copy = pltpu.make_async_copy(kc_hbm.at[1], kbuf, kv_sem.at[0])
    v_copy = pltpu.make_async_copy(vc_hbm.at[1], vbuf, kv_sem.at[1])
    for n in range(NCH):
        dense_copy(0, n).start()
    for n in range(NCH):
        up_copy(0, n).start()
    for n in range(NCH):
        down_copy(0, n).start()
    for n in range(NCH):
        qkv_copy(n).start()
    k_copy.start()
    v_copy.start()

    my_rows = pl.ds(pl.multiple_of(s * ROWS, ROWS), ROWS)
    wide = hidden[my_rows, :].astype(F32)
    for j in range(4):
        x_all[j] = wide[OWN * j:OWN * (j + 1)]
    x_own[...] = x_all[t]
    q8[...] = jnp.zeros_like(q8)
    pl.semaphore_wait(barrier, 6)

    def exchange(layer, stats):
        for d in range(1, 4):
            peer = lax.rem(s + d, 4)
            rows = pl.ds(pl.multiple_of(peer * ROWS, ROWS), ROWS)
            send(stats.at[rows], mix.at[layer, d - 1], mix_send.at[layer, d - 1], mix_recv.at[layer, d - 1], "sp", peer)

    def combine(layer, stats, qkv_rows):
        for d in range(1, 4):
            arrived(mix.at[layer, d - 1], mix_send.at[layer, d - 1], mix_recv.at[layer, d - 1], "sp", lax.rem(s + d, 4))
        shards = [stats[my_rows, :]] + [mix[layer, d] for d in range(3)]
        for h in range(HEADS):
            base = h // GROUP * 5
            q = qkv_rows[:, (base + h % GROUP) * HEAD:(base + h % GROUP + 1) * HEAD]
            k = qkv_rows[:, (base + GROUP) * HEAD:(base + GROUP + 1) * HEAD]
            v = qkv_rows[:, (base + GROUP + 1) * HEAD:(base + GROUP + 2) * HEAD]
            fresh = jnp.sum(q * k, axis=-1, keepdims=True) * (1.0 / HEAD)
            peaks = [x[:, HEADS * HEAD + h:HEADS * HEAD + h + 1] for x in shards]
            top = fresh
            for peak in peaks:
                top = jnp.maximum(top, peak)
            scale = jnp.exp(fresh - top)
            num, den = v * scale, scale
            for x, peak in zip(shards, peaks):
                scale = jnp.exp(peak - top)
                num = num + x[:, h * HEAD:(h + 1) * HEAD] * scale
                den = den + x[:, HEADS * HEAD + HEADS + h:HEADS * HEAD + HEADS + h + 1] * scale
            o16[:, h * HEAD:(h + 1) * HEAD] = (num / den).astype(BF16)

    def reduce_rows(phase, lhs, weights, layer, copy_of, reload):
        for n in range(NCH):
            copy_of(layer, n).wait()
            piece = dot(lhs[...], weights[:, n * CH:(n + 1) * CH])
            for j in range(4):
                part[phase, j, :, n * CH:(n + 1) * CH] = piece[OWN * j:OWN * (j + 1)]
            for d in range(1, 4):
                peer = lax.rem(t + d, 4)
                send(part.at[phase, peer, :, cols[n]], summed.at[phase, d - 1, :, cols[n]],
                     part_send.at[phase, d - 1, n], part_recv.at[phase, d - 1, n], "tp", peer)
            if reload:
                copy_of(layer + 1, n).start()
        for n in range(NCH):
            for d in range(1, 4):
                arrived(summed.at[phase, d - 1, :, cols[n]], part_send.at[phase, d - 1, n],
                        part_recv.at[phase, d - 1, n], "tp", lax.rem(t + d, 4))
        return part[phase, t] + summed[phase, 0] + summed[phase, 1] + summed[phase, 2]

    def spread_rows(phase, rows):
        spread[phase, t] = rows.astype(F32)
        for n in range(NCH):
            for d in range(1, 4):
                send(spread.at[phase, t, :, cols[n]], spread.at[phase, t, :, cols[n]],
                     spread_send.at[phase, d - 1, n], spread_recv.at[phase, d - 1, n], "tp", lax.rem(t + d, 4))

    def take_rows(phase, n):
        for d in range(1, 4):
            arrived(spread.at[phase, lax.rem(t - d + 4, 4), :, cols[n]], spread_send.at[phase, d - 1, n],
                    spread_recv.at[phase, d - 1, n], "tp", lax.rem(t + d, 4))
        rows = [spread[phase, j, :, n * CH:(n + 1) * CH] for j in range(4)]
        u16[...] = jnp.concatenate(rows, axis=0).astype(BF16)

    lane = lax.broadcasted_iota(jnp.int32, (ROWS, 1024), 1)
    pick = (lax.broadcasted_iota(jnp.int32, (256, 128), 0) == 2 * lax.broadcasted_iota(jnp.int32, (256, 128), 1))
    pick = jnp.where(pick, 1.0, 0.0).astype(BF16)

    def finish_layer(layer):
        last = layer == 1
        total = reduce_rows(2 * layer, o16, wdense, layer, dense_copy, not last)
        x1 = round_bf16(x_own[...] + total + param_row(b_dense, layer))
        x_own[...] = x1
        spread_rows(2 * layer, norm_rows(x1, param_row(gain, layer, 1), param_row(shift, layer, 1)))
        bias = param_row(b_up, layer)
        for n in range(NCH):
            up_copy(layer, n).wait()
            take_rows(2 * layer, n)
            for c in range(4):
                at = slice(c * 1024, (c + 1) * 1024)
                piece = dot(u16[...], wup[n * CH:(n + 1) * CH, at])
                h_s[:, at] = piece + bias[:, at] if n == 0 else h_s[:, at] + piece
            if not last:
                up_copy(layer + 1, n).start()
        for c in range(4):
            pair = h_s[:, c * 1024:(c + 1) * 1024]
            gate = jnp.minimum(pair, GELU_LIMIT)
            line = jnp.clip(pltpu.roll(pair, 1023, 1), -GELU_LIMIT, GELU_LIMIT)
            act = gate * jax.nn.sigmoid(1.702 * gate) * (line + 1.0)
            act = jnp.where(lane % 2 == 0, act, 0.0).astype(BF16)
            for k in range(4):
                at = slice(c * 512 + k * 128, c * 512 + (k + 1) * 128)
                m16[:, at] = dot(act[:, k * 256:(k + 1) * 256], pick).astype(BF16)
        total = reduce_rows(2 * layer + 1, m16, wdown, layer, down_copy, not last)
        x_own[...] = round_bf16(x_own[...] + total + param_row(b_down, layer))

    exchange(0, stats0)
    combine(0, stats0, qkv0[my_rows, :])
    finish_layer(0)

    spread_rows(1, norm_rows(x_own[...], param_row(gain, 1, 0), param_row(shift, 1, 0)))
    mine = qkv1.at[s]
    for n in range(NCH):
        qkv_copy(n).wait()
        take_rows(1, n)
        piece = dot(u16[...], wqkv[n * CH:(n + 1) * CH, :])
        mine[...] = piece + param_row(b_qkv, 1) if n == 0 else mine[...] + piece
    turn_columns(mine, slice(None), cos_rows[my_rows, :], sin_rows[my_rows, :])
    for d in range(1, 4):
        send(mine, mine, q_send.at[d - 1], q_recv.at[d - 1], "sp", lax.rem(s + d, 4))
    for d in range(1, 4):
        arrived(qkv1.at[lax.rem(s - d + 4, 4)], q_send.at[d - 1], q_recv.at[d - 1], "sp", lax.rem(s + d, 4))
    for i in range(4):
        for h in range(HEADS):
            at = (h // GROUP * 5 + h % GROUP) * HEAD
            q8[pl.ds(i * ROWS * 8 + h, ROWS, stride=8), :] = qkv1[i, :, at:at + HEAD]
        qkv1_out[i * ROWS:(i + 1) * ROWS, :] = qkv1[i]
    k_copy.wait()
    v_copy.wait()

    def one_group(g, carry):
        attend(g, False, pos_ref, q8, kbuf, vbuf, acc8, m8, l8)
        return carry

    lax.fori_loop(0, NGRP, one_group, 0)
    pack_stats(stats1, acc8, m8, l8)
    exchange(1, stats1)
    combine(1, stats1, qkv1[s])
    finish_layer(1)

    twin = s + 1 - 2 * lax.rem(s, 2)
    across = lax.rem(s + 2, 4)
    fin[s, t] = x_own[...]

    def forward(block, kind, index, axis, peer):
        send(block, block, fin_send.at[kind, index], fin_recv.at[kind, index], axis, peer)

    def landed(block, kind, index, axis, peer):
        arrived(block, fin_send.at[kind, index], fin_recv.at[kind, index], axis, peer)

    for d in range(1, 4):
        forward(fin.at[s, t], 0, d, "tp", lax.rem(t + d, 4))
    forward(fin.at[s, t], 1, 0, "sp", across)
    forward(fin.at[s, t], 2, 0, "sp", twin)
    for d in range(1, 4):
        block = fin.at[s, lax.rem(t - d + 4, 4)]
        landed(block, 0, d, "tp", lax.rem(t + d, 4))
        forward(block, 1, d, "sp", across)
        forward(block, 2, d, "sp", twin)
    for d in range(4):
        block = fin.at[across, lax.rem(t - d + 4, 4)]
        landed(block, 1, d, "sp", across)
        forward(block, 3, d, "sp", twin)
    diagonal = lax.rem(twin + 2, 4)
    for d in range(4):
        landed(fin.at[twin, lax.rem(t - d + 4, 4)], 2, d, "sp", twin)
        landed(fin.at[diagonal, lax.rem(t - d + 4, 4)], 3, d, "sp", twin)
    for i in range(4):
        rows = jnp.concatenate([fin[i, j] for j in range(4)], axis=0)
        hid[i * ROWS:(i + 1) * ROWS, :] = rows.astype(BF16)
    for copy in sends:
        copy.wait_send()


def solution(mesh):
    cache_spec = P(None, "dp", "sp", "tp", None)
    in_specs = (P("dp", None), P("dp"), cache_spec, cache_spec, P(), P(), P(None, None, "tp"), P(None, "tp"),
                P(None, "tp", None), P(), P(None, None, "tp"), P(None, "tp"), P(None, "tp", None), P())
    out_specs = (P("dp", None), cache_spec, cache_spec)
    cos_np, sin_np = rope_tables()
    vmem, smem, hbm = (pl.BlockSpec(memory_space=m) for m in (pltpu.VMEM, pltpu.SMEM, pl.ANY))
    dma = pltpu.SemaphoreType.DMA

    def device_step(hidden, positions, k_cache, v_cache, ln_gain, ln_bias, w_qkv, b_qkv, w_dense, b_dense,
                    w_up, b_up, w_down, b_down):
        flat = (2, SEQS, SLOTS * KV, HEAD)
        kc, vc = k_cache.reshape(flat), v_cache.reshape(flat)
        cache = jax.ShapeDtypeStruct(flat, BF16)
        kv_buffers = [pltpu.VMEM(flat[1:], BF16)] * 2
        row8 = [pltpu.VMEM((SEQS * 8, HEAD), F32)] * 4
        ko, vo, qkv0, stats0, cos_rows, sin_rows = pl.pallas_call(
            entry_kernel,
            out_shape=(cache, cache, jax.ShapeDtypeStruct((SEQS, QKV), F32), jax.ShapeDtypeStruct((SEQS, STAT), F32),
                       jax.ShapeDtypeStruct((SEQS, HEAD), F32), jax.ShapeDtypeStruct((SEQS, HEAD), F32)),
            in_specs=[smem] + [vmem] * 6 + [hbm] * 3,
            out_specs=(hbm, hbm, vmem, vmem, vmem, vmem),
            scratch_shapes=[pltpu.VMEM((D, QKV), BF16)] + kv_buffers + [pltpu.VMEM((SEQS, D), BF16)] + row8
            + [dma((NCH,))] + [dma((NGRP,))] * 4,
            compiler_params=pltpu.CompilerParams(vmem_limit_bytes=VMEM_MAX),
            name="entry",
        )(positions, hidden, ln_gain, ln_bias, b_qkv, cos_np, sin_np, w_qkv, kc, vc)

        hid, qkv1 = pl.pallas_call(
            main_kernel,
            out_shape=(jax.ShapeDtypeStruct((SEQS, D), BF16), jax.ShapeDtypeStruct((SEQS, QKV), F32)),
            in_specs=[smem] + [vmem] * 11 + [hbm] * 6,
            out_specs=(vmem, vmem),
            scratch_shapes=[
                pltpu.VMEM((D, QKV), BF16), pltpu.VMEM((HEADS * HEAD, D), BF16), pltpu.VMEM((D, UP), BF16),
                pltpu.VMEM((FF, D), BF16)] + kv_buffers + [
                pltpu.VMEM((2, 3, ROWS, STAT), F32),
                pltpu.VMEM((4, 4, OWN, D), F32),
                pltpu.VMEM((4, 3, OWN, D), F32),
                pltpu.VMEM((3, 4, OWN, D), F32),
                pltpu.VMEM((OWN, D), F32),
                pltpu.VMEM((4, OWN, D), F32),
                pltpu.VMEM((ROWS, HEADS * HEAD), BF16),
                pltpu.VMEM((ROWS, CH), BF16),
                pltpu.VMEM((ROWS, UP), F32),
                pltpu.VMEM((ROWS, FF), BF16),
                pltpu.VMEM((4, ROWS, QKV), F32),
                pltpu.VMEM((SEQS, STAT), F32),
                pltpu.VMEM((4, 4, OWN, D), F32),
            ] + row8 + [
                dma((4, NCH)), dma((2,)), dma((2, 3)), dma((2, 3)), dma((4, 3, NCH)), dma((4, 3, NCH)),
                dma((3, 3, NCH)), dma((3, 3, NCH)), dma((3,)), dma((3,)), dma((4, 4)), dma((4, 4))],
            compiler_params=pltpu.CompilerParams(vmem_limit_bytes=VMEM_MAX, collective_id=0, has_side_effects=True),
            name="main",
        )(positions, stats0, qkv0, cos_rows, sin_rows, hidden, ln_gain, ln_bias, b_qkv, b_dense, b_up, b_down,
          w_qkv, w_dense, w_up, w_down, kc, vc)

        hidden_out, ko, vo = pl.pallas_call(
            exit_kernel,
            out_shape=(jax.ShapeDtypeStruct((SEQS, D), BF16), cache, cache),
            in_specs=[smem, vmem, vmem] + [hbm] * 4,
            out_specs=(vmem, hbm, hbm),
            scratch_shapes=kv_buffers + [dma((NGRP,))] * 4,
            input_output_aliases={5: 1, 6: 2},
            compiler_params=pltpu.CompilerParams(vmem_limit_bytes=VMEM_MAX),
            name="exit",
        )(positions, qkv1, hid, kc, vc, ko, vo)
        return hidden_out, ko.reshape(k_cache.shape), vo.reshape(v_cache.shape)

    return jax.shard_map(device_step, mesh=mesh, in_specs=in_specs, out_specs=out_specs, check_vma=False)
```

```python
import functools

import jax
import jax.numpy as jnp
import numpy as np
from jax import lax
from jax.experimental import pallas as pl
from jax.experimental.pallas import tpu as pltpu
from jax.sharding import PartitionSpec as P

MESH = pl.DeviceIdType.MESH
F32 = jnp.float32
BF16 = jnp.bfloat16
BLOCK_SIZE = 64
LOCAL_BLOCKS = 16
VERT_STRIDE = 8
ROPE_THETA = 1000000.0
GELU_LIMIT = 20.0
NORM_EPS = 0.00001
MASKED = -1e30

SEQS = 64
ROWS = 16
OWN = 4
SEQ_LEN = 512
SLOTS = 128
D = 3072
HEAD = 128
KV = 2
GROUP = 3
HEADS = KV * GROUP
QKV = 1280
UP = 4096
FF = 2048
STAT = HEADS * HEAD + HEAD
NCH = 3
CH = D // NCH
GRP = 8
NGRP = SEQS // GRP
VMEM_MAX = 67043328


def rope_tables():
    half = HEAD // 2
    inv = (ROPE_THETA ** (-np.arange(half).astype(np.float32) * np.float32(2.0 / HEAD))).astype(np.float32)
    angle = (np.arange(SEQ_LEN).astype(np.float32)[:, None] * inv[None, :]).astype(np.float64)
    cos, sin = np.cos(angle).astype(np.float32), np.sin(angle).astype(np.float32)
    return np.concatenate([cos, cos], 1), np.concatenate([-sin, sin], 1)


def norm_rows(wide, gain, shift):
    mean = jnp.mean(wide, axis=-1, keepdims=True)
    centred = wide - mean
    var = jnp.mean(centred * centred, axis=-1, keepdims=True)
    return (centred * lax.rsqrt(var + NORM_EPS) * gain + shift).astype(BF16)


def param_row(ref, layer, which=None):
    rows = ref[...] if which is None else ref[layer]
    pick = layer if which is None else which
    return rows.astype(F32)[pick:pick + 1]


def round_bf16(x):
    return x.astype(BF16).astype(F32)


def dot(a, b):
    return jnp.dot(a, b, preferred_element_type=F32)


def turn_columns(ref, rows, cos, sin):
    for c in range(KV):
        for g in range(GROUP + 2):
            cols = slice((c * 5 + g) * HEAD, (c * 5 + g + 1) * HEAD)
            x = ref[rows, cols]
            if g <= GROUP:
                x = x * cos + pltpu.roll(x, HEAD // 2, 1) * sin
            ref[rows, cols] = round_bf16(x)


def attend(sparse, pos_ref, q8, kbuf, vbuf, s8, acc8, m8, l8):
    t, s = lax.axis_index("tp"), lax.axis_index("sp")
    row = lax.broadcasted_iota(jnp.int32, (8, KV * SLOTS), 0)
    col = lax.broadcasted_iota(jnp.int32, (8, KV * SLOTS), 1)
    slot = s * SLOTS + col // KV
    same = (col % KV) == row // GROUP
    vertical = (slot // BLOCK_SIZE + (t * HEADS + row) + 1) % VERT_STRIDE == 0
    for b in range(SEQS):
        at = slice(b * 8, b * 8 + 8)
        p = pos_ref[b]
        scores = lax.dot_general(q8[at, :].astype(BF16), kbuf[b], (((1,), (1,)), ((), ())), preferred_element_type=F32)
        keep = (slot < p) & same
        if sparse:
            near = (p // BLOCK_SIZE - slot // BLOCK_SIZE) < LOCAL_BLOCKS
            keep = keep & (near | vertical)
        s8[at, :] = jnp.where(keep, scores * (1.0 / HEAD), -jnp.inf)
    for r in range(8):
        at = slice(r * SEQS, (r + 1) * SEQS)
        scores = s8[at, :]
        peak = jnp.maximum(jnp.max(scores, axis=-1, keepdims=True), MASKED)
        weights = jnp.exp(scores - peak)
        s8[at, :] = weights
        m8[at, :] = jnp.broadcast_to(peak, (SEQS, HEAD))
        l8[at, :] = jnp.broadcast_to(jnp.sum(weights, axis=-1, keepdims=True), (SEQS, HEAD))
    for b in range(SEQS):
        at = slice(b * 8, b * 8 + 8)
        acc8[at, :] = dot(s8[at, :].astype(BF16), vbuf[b])


def pack_stats(stats, acc8, m8, l8):
    lane = lax.broadcasted_iota(jnp.int32, (SEQS, HEAD), 1)
    tail = jnp.zeros((SEQS, HEAD), F32)
    for h in range(HEADS):
        at = pl.ds(h, SEQS, stride=8)
        stats[:, h * HEAD:(h + 1) * HEAD] = acc8[at, :]
        tail = jnp.where(lane == h, m8[at, :], tail)
        tail = jnp.where(lane == HEADS + h, l8[at, :], tail)
    stats[:, HEADS * HEAD:] = tail


def put_new_rows(group, pos_ref, qkv_ref, kbuf, vbuf):
    s = lax.axis_index("sp")
    row = lax.broadcasted_iota(jnp.int32, (16, HEAD), 0)
    group_rows = pl.ds(pl.multiple_of(group * GRP, GRP), GRP)
    pairs = [[qkv_ref[group_rows, (5 * c + which) * HEAD:(5 * c + which + 1) * HEAD] for c in range(KV)]
             for which in (GROUP, GROUP + 1)]
    for j in range(GRP):
        b = group * GRP + j
        local = pos_ref[b] - s * SLOTS
        inside = jnp.where((local >= 0) & (local < SLOTS), 1, 0)
        local = jnp.clip(local, 0, SLOTS - 1)
        at = pl.ds(pl.multiple_of((local // 8) * 16, 16), 16)
        target = jnp.where(inside == 1, local % 8, 99)
        hit = (row // KV) == target
        for buf, (first, second) in zip((kbuf, vbuf), pairs):
            fresh = jnp.where(row % KV == 0, first[j:j + 1], second[j:j + 1])
            buf[b, at, :] = jnp.where(hit, fresh, buf[b, at, :].astype(F32)).astype(BF16)


def entry_kernel(pos_ref, hidden, gain, shift, b_qkv, cos, sin, w_hbm, kc_hbm, vc_hbm,
                 ko_hbm, vo_hbm, qkv, stats, cos_rows, sin_rows,
                 wbuf, kbuf, vbuf, u_s, q8, s8, acc8, m8, l8, wsem, ksem, vsem, kosem, vosem):
    def w_copy(i):
        return pltpu.make_async_copy(w_hbm.at[0, pl.ds(i * CH, CH)], wbuf.at[pl.ds(i * CH, CH)], wsem.at[i])

    def in_copies(g):
        at = pl.ds(g * GRP, GRP)
        return (pltpu.make_async_copy(kc_hbm.at[0, at], kbuf.at[at], ksem.at[g]),
                pltpu.make_async_copy(vc_hbm.at[0, at], vbuf.at[at], vsem.at[g]))

    def out_copies(g):
        at = pl.ds(g * GRP, GRP)
        return (pltpu.make_async_copy(kbuf.at[at], ko_hbm.at[0, at], kosem.at[g]),
                pltpu.make_async_copy(vbuf.at[at], vo_hbm.at[0, at], vosem.at[g]))

    for i in range(NCH):
        w_copy(i).start()
    for g in range(NGRP):
        for copy in in_copies(g):
            copy.start()

    def pick_row(b, carry):
        p = pos_ref[b]
        cos_rows[pl.ds(b, 1), :] = cos[pl.ds(p, 1), :]
        sin_rows[pl.ds(b, 1), :] = sin[pl.ds(p, 1), :]
        return carry

    lax.fori_loop(0, SEQS, pick_row, 0)
    q8[...] = jnp.zeros_like(q8)
    u_s[...] = norm_rows(hidden[...].astype(F32), param_row(gain, 0, 0), param_row(shift, 0, 0))
    for i in range(NCH):
        w_copy(i).wait()
        piece = dot(u_s[:, i * CH:(i + 1) * CH], wbuf[i * CH:(i + 1) * CH, :])
        qkv[...] = piece + param_row(b_qkv, 0) if i == 0 else qkv[...] + piece
    turn_columns(qkv, slice(None), cos_rows[...], sin_rows[...])
    for h in range(HEADS):
        cols = (h // GROUP * 5 + h % GROUP) * HEAD
        q8[pl.ds(h, SEQS, stride=8), :] = qkv[:, cols:cols + HEAD]

    def one_group(g, carry):
        for copy in in_copies(g):
            copy.wait()
        put_new_rows(g, pos_ref, qkv, kbuf, vbuf)
        for copy in out_copies(g):
            copy.start()
        return carry

    lax.fori_loop(0, NGRP, one_group, 0)
    attend(True, pos_ref, q8, kbuf, vbuf, s8, acc8, m8, l8)
    pack_stats(stats, acc8, m8, l8)

    def drain(g, carry):
        for copy in out_copies(g):
            copy.wait()
        return carry

    lax.fori_loop(0, NGRP, drain, 0)


def exit_kernel(pos_ref, qkv, hid, kc_hbm, vc_hbm, ka_hbm, va_hbm, hid_out, ko_hbm, vo_hbm,
                kbuf, vbuf, ksem, vsem, kosem, vosem):
    def in_copies(g):
        at = pl.ds(g * GRP, GRP)
        return (pltpu.make_async_copy(kc_hbm.at[1, at], kbuf.at[at], ksem.at[g]),
                pltpu.make_async_copy(vc_hbm.at[1, at], vbuf.at[at], vsem.at[g]))

    def out_copies(g):
        at = pl.ds(g * GRP, GRP)
        return (pltpu.make_async_copy(kbuf.at[at], ko_hbm.at[1, at], kosem.at[g]),
                pltpu.make_async_copy(vbuf.at[at], vo_hbm.at[1, at], vosem.at[g]))

    for g in range(NGRP):
        for copy in in_copies(g):
            copy.start()
    hid_out[...] = hid[...]

    def one_group(g, carry):
        for copy in in_copies(g):
            copy.wait()
        put_new_rows(g, pos_ref, qkv, kbuf, vbuf)
        for copy in out_copies(g):
            copy.start()
        return carry

    lax.fori_loop(0, NGRP, one_group, 0)

    def drain(g, carry):
        for copy in out_copies(g):
            copy.wait()
        return carry

    lax.fori_loop(0, NGRP, drain, 0)


def main_kernel(pos_ref, stats0, qkv0, cos_rows, sin_rows, hidden, gain, shift, b_qkv, b_dense, b_up, b_down,
                wqkv_hbm, wdense_hbm, wup_hbm, wdown_hbm, kc_hbm, vc_hbm,
                hid, qkv1_out,
                wqkv, wdense, wup, wdown, kbuf, vbuf,
                mix, part, summed, spread, x_own, x_all, o16, u16, h_s, m16, qkv1, stats1, fin, q8, s8, acc8, m8, l8,
                w_sem, kv_sem, mix_send, mix_recv, part_send, part_recv, spread_send, spread_recv,
                q_send, q_recv, fin_send, fin_recv):
    t, s = lax.axis_index("tp"), lax.axis_index("sp")
    sends = []

    def send(src, dst, send_sem, recv_sem, axis, peer):
        copy = pltpu.make_async_remote_copy(src_ref=src, dst_ref=dst, send_sem=send_sem, recv_sem=recv_sem,
                                            device_id={axis: peer}, device_id_type=MESH)
        copy.start()
        sends.append(copy)

    def arrived(dst, send_sem, recv_sem, axis, peer):
        pltpu.make_async_remote_copy(src_ref=dst, dst_ref=dst, send_sem=send_sem, recv_sem=recv_sem,
                                     device_id={axis: peer}, device_id_type=MESH).wait_recv()

    barrier = pltpu.get_barrier_semaphore()
    for axis, me in (("tp", t), ("sp", s)):
        for d in range(1, 4):
            pl.semaphore_signal(barrier, inc=1, device_id={axis: lax.rem(me + d, 4)}, device_id_type=MESH)

    cols = [pl.ds(n * CH, CH) for n in range(NCH)]

    def dense_copy(layer, n):
        return pltpu.make_async_copy(wdense_hbm.at[layer, :, cols[n]], wdense.at[:, cols[n]], w_sem.at[0, n])

    def up_copy(layer, n):
        return pltpu.make_async_copy(wup_hbm.at[layer, cols[n]], wup.at[cols[n]], w_sem.at[1, n])

    def down_copy(layer, n):
        return pltpu.make_async_copy(wdown_hbm.at[layer, :, cols[n]], wdown.at[:, cols[n]], w_sem.at[2, n])

    def qkv_copy(n):
        return pltpu.make_async_copy(wqkv_hbm.at[1, cols[n]], wqkv.at[cols[n]], w_sem.at[3, n])

    k_copy = pltpu.make_async_copy(kc_hbm.at[1], kbuf, kv_sem.at[0])
    v_copy = pltpu.make_async_copy(vc_hbm.at[1], vbuf, kv_sem.at[1])
    for n in range(NCH):
        dense_copy(0, n).start()
    for n in range(NCH):
        up_copy(0, n).start()
    for n in range(NCH):
        down_copy(0, n).start()
    for n in range(NCH):
        qkv_copy(n).start()
    k_copy.start()
    v_copy.start()

    my_rows = pl.ds(pl.multiple_of(s * ROWS, ROWS), ROWS)
    wide = hidden[my_rows, :].astype(F32)
    for j in range(4):
        x_all[j] = wide[OWN * j:OWN * (j + 1)]
    x_own[...] = x_all[t]
    q8[...] = jnp.zeros_like(q8)
    pl.semaphore_wait(barrier, 6)

    def exchange(layer, stats):
        for d in range(1, 4):
            peer = lax.rem(s + d, 4)
            rows = pl.ds(pl.multiple_of(peer * ROWS, ROWS), ROWS)
            send(stats.at[rows], mix.at[layer, d - 1], mix_send.at[layer, d - 1], mix_recv.at[layer, d - 1], "sp", peer)

    def combine(layer, stats, qkv_rows):
        for d in range(1, 4):
            arrived(mix.at[layer, d - 1], mix_send.at[layer, d - 1], mix_recv.at[layer, d - 1], "sp", lax.rem(s + d, 4))
        shards = [stats[my_rows, :]] + [mix[layer, d] for d in range(3)]
        for h in range(HEADS):
            base = h // GROUP * 5
            q = qkv_rows[:, (base + h % GROUP) * HEAD:(base + h % GROUP + 1) * HEAD]
            k = qkv_rows[:, (base + GROUP) * HEAD:(base + GROUP + 1) * HEAD]
            v = qkv_rows[:, (base + GROUP + 1) * HEAD:(base + GROUP + 2) * HEAD]
            fresh = jnp.sum(q * k, axis=-1, keepdims=True) * (1.0 / HEAD)
            peaks = [x[:, HEADS * HEAD + h:HEADS * HEAD + h + 1] for x in shards]
            top = fresh
            for peak in peaks:
                top = jnp.maximum(top, peak)
            scale = jnp.exp(fresh - top)
            num, den = v * scale, scale
            for x, peak in zip(shards, peaks):
                scale = jnp.exp(peak - top)
                num = num + x[:, h * HEAD:(h + 1) * HEAD] * scale
                den = den + x[:, HEADS * HEAD + HEADS + h:HEADS * HEAD + HEADS + h + 1] * scale
            o16[:, h * HEAD:(h + 1) * HEAD] = (num / den).astype(BF16)

    def reduce_rows(phase, lhs, weights, layer, copy_of, reload):
        for n in range(NCH):
            copy_of(layer, n).wait()
            piece = dot(lhs[...], weights[:, n * CH:(n + 1) * CH])
            for j in range(4):
                part[phase, j, :, n * CH:(n + 1) * CH] = piece[OWN * j:OWN * (j + 1)]
            for d in range(1, 4):
                peer = lax.rem(t + d, 4)
                send(part.at[phase, peer, :, cols[n]], summed.at[phase, d - 1, :, cols[n]],
                     part_send.at[phase, d - 1, n], part_recv.at[phase, d - 1, n], "tp", peer)
            if reload:
                copy_of(layer + 1, n).start()
        for n in range(NCH):
            for d in range(1, 4):
                arrived(summed.at[phase, d - 1, :, cols[n]], part_send.at[phase, d - 1, n],
                        part_recv.at[phase, d - 1, n], "tp", lax.rem(t + d, 4))
        return part[phase, t] + summed[phase, 0] + summed[phase, 1] + summed[phase, 2]

    def spread_rows(phase, rows):
        spread[phase, t] = rows.astype(F32)
        for n in range(NCH):
            for d in range(1, 4):
                send(spread.at[phase, t, :, cols[n]], spread.at[phase, t, :, cols[n]],
                     spread_send.at[phase, d - 1, n], spread_recv.at[phase, d - 1, n], "tp", lax.rem(t + d, 4))

    def take_rows(phase, n):
        for d in range(1, 4):
            arrived(spread.at[phase, lax.rem(t - d + 4, 4), :, cols[n]], spread_send.at[phase, d - 1, n],
                    spread_recv.at[phase, d - 1, n], "tp", lax.rem(t + d, 4))
        rows = [spread[phase, j, :, n * CH:(n + 1) * CH] for j in range(4)]
        u16[...] = jnp.concatenate(rows, axis=0).astype(BF16)

    lane = lax.broadcasted_iota(jnp.int32, (ROWS, 1024), 1)
    pick = (lax.broadcasted_iota(jnp.int32, (256, 128), 0) == 2 * lax.broadcasted_iota(jnp.int32, (256, 128), 1))
    pick = jnp.where(pick, 1.0, 0.0).astype(BF16)

    def finish_layer(layer):
        last = layer == 1
        total = reduce_rows(2 * layer, o16, wdense, layer, dense_copy, not last)
        x1 = round_bf16(x_own[...] + total + param_row(b_dense, layer))
        x_own[...] = x1
        spread_rows(2 * layer, norm_rows(x1, param_row(gain, layer, 1), param_row(shift, layer, 1)))
        bias = param_row(b_up, layer)
        for n in range(NCH):
            up_copy(layer, n).wait()
            take_rows(2 * layer, n)
            for c in range(4):
                at = slice(c * 1024, (c + 1) * 1024)
                piece = dot(u16[...], wup[n * CH:(n + 1) * CH, at])
                h_s[:, at] = piece + bias[:, at] if n == 0 else h_s[:, at] + piece
            if not last:
                up_copy(layer + 1, n).start()
        for c in range(4):
            pair = h_s[:, c * 1024:(c + 1) * 1024]
            gate = jnp.minimum(pair, GELU_LIMIT)
            line = jnp.clip(pltpu.roll(pair, 1023, 1), -GELU_LIMIT, GELU_LIMIT)
            act = gate * jax.nn.sigmoid(1.702 * gate) * (line + 1.0)
            act = jnp.where(lane % 2 == 0, act, 0.0).astype(BF16)
            for k in range(4):
                at = slice(c * 512 + k * 128, c * 512 + (k + 1) * 128)
                m16[:, at] = dot(act[:, k * 256:(k + 1) * 256], pick).astype(BF16)
        total = reduce_rows(2 * layer + 1, m16, wdown, layer, down_copy, not last)
        x_own[...] = round_bf16(x_own[...] + total + param_row(b_down, layer))

    exchange(0, stats0)
    combine(0, stats0, qkv0[my_rows, :])
    finish_layer(0)

    spread_rows(1, norm_rows(x_own[...], param_row(gain, 1, 0), param_row(shift, 1, 0)))
    mine = qkv1.at[s]
    for n in range(NCH):
        qkv_copy(n).wait()
        take_rows(1, n)
        piece = dot(u16[...], wqkv[n * CH:(n + 1) * CH, :])
        mine[...] = piece + param_row(b_qkv, 1) if n == 0 else mine[...] + piece
    turn_columns(mine, slice(None), cos_rows[my_rows, :], sin_rows[my_rows, :])
    for d in range(1, 4):
        send(mine, mine, q_send.at[d - 1], q_recv.at[d - 1], "sp", lax.rem(s + d, 4))
    for d in range(1, 4):
        arrived(qkv1.at[lax.rem(s - d + 4, 4)], q_send.at[d - 1], q_recv.at[d - 1], "sp", lax.rem(s + d, 4))
    for i in range(4):
        for h in range(HEADS):
            at = (h // GROUP * 5 + h % GROUP) * HEAD
            q8[pl.ds(i * ROWS * 8 + h, ROWS, stride=8), :] = qkv1[i, :, at:at + HEAD]
        qkv1_out[i * ROWS:(i + 1) * ROWS, :] = qkv1[i]
    k_copy.wait()
    v_copy.wait()

    attend(False, pos_ref, q8, kbuf, vbuf, s8, acc8, m8, l8)
    pack_stats(stats1, acc8, m8, l8)
    exchange(1, stats1)
    combine(1, stats1, qkv1[s])
    finish_layer(1)

    twin = s + 1 - 2 * lax.rem(s, 2)
    across = lax.rem(s + 2, 4)
    fin[s, t] = x_own[...]

    def forward(block, kind, index, axis, peer):
        send(block, block, fin_send.at[kind, index], fin_recv.at[kind, index], axis, peer)

    def landed(block, kind, index, axis, peer):
        arrived(block, fin_send.at[kind, index], fin_recv.at[kind, index], axis, peer)

    for d in range(1, 4):
        forward(fin.at[s, t], 0, d, "tp", lax.rem(t + d, 4))
    forward(fin.at[s, t], 1, 0, "sp", across)
    forward(fin.at[s, t], 2, 0, "sp", twin)
    for d in range(1, 4):
        block = fin.at[s, lax.rem(t - d + 4, 4)]
        landed(block, 0, d, "tp", lax.rem(t + d, 4))
        forward(block, 1, d, "sp", across)
        forward(block, 2, d, "sp", twin)
    for d in range(4):
        block = fin.at[across, lax.rem(t - d + 4, 4)]
        landed(block, 1, d, "sp", across)
        forward(block, 3, d, "sp", twin)
    diagonal = lax.rem(twin + 2, 4)
    for d in range(4):
        landed(fin.at[twin, lax.rem(t - d + 4, 4)], 2, d, "sp", twin)
        landed(fin.at[diagonal, lax.rem(t - d + 4, 4)], 3, d, "sp", twin)
    for i in range(4):
        rows = jnp.concatenate([fin[i, j] for j in range(4)], axis=0)
        hid[i * ROWS:(i + 1) * ROWS, :] = rows.astype(BF16)
    for copy in sends:
        copy.wait_send()


def solution(mesh):
    cache_spec = P(None, "dp", "sp", "tp", None)
    in_specs = (P("dp", None), P("dp"), cache_spec, cache_spec, P(), P(), P(None, None, "tp"), P(None, "tp"),
                P(None, "tp", None), P(), P(None, None, "tp"), P(None, "tp"), P(None, "tp", None), P())
    out_specs = (P("dp", None), cache_spec, cache_spec)
    cos_np, sin_np = rope_tables()
    vmem, smem, hbm = (pl.BlockSpec(memory_space=m) for m in (pltpu.VMEM, pltpu.SMEM, pl.ANY))
    dma = pltpu.SemaphoreType.DMA

    def device_step(hidden, positions, k_cache, v_cache, ln_gain, ln_bias, w_qkv, b_qkv, w_dense, b_dense,
                    w_up, b_up, w_down, b_down):
        flat = (2, SEQS, SLOTS * KV, HEAD)
        kc, vc = k_cache.reshape(flat), v_cache.reshape(flat)
        cache = jax.ShapeDtypeStruct(flat, BF16)
        kv_buffers = [pltpu.VMEM(flat[1:], BF16)] * 2
        row8 = [pltpu.VMEM((SEQS * 8, n * HEAD), F32) for n in (1, 2, 1, 1, 1)]
        ko, vo, qkv0, stats0, cos_rows, sin_rows = pl.pallas_call(
            entry_kernel,
            out_shape=(cache, cache, jax.ShapeDtypeStruct((SEQS, QKV), F32), jax.ShapeDtypeStruct((SEQS, STAT), F32),
                       jax.ShapeDtypeStruct((SEQS, HEAD), F32), jax.ShapeDtypeStruct((SEQS, HEAD), F32)),
            in_specs=[smem] + [vmem] * 6 + [hbm] * 3,
            out_specs=(hbm, hbm, vmem, vmem, vmem, vmem),
            scratch_shapes=[pltpu.VMEM((D, QKV), BF16)] + kv_buffers + [pltpu.VMEM((SEQS, D), BF16)] + row8
            + [dma((NCH,))] + [dma((NGRP,))] * 4,
            compiler_params=pltpu.CompilerParams(vmem_limit_bytes=VMEM_MAX),
            name="entry",
        )(positions, hidden, ln_gain, ln_bias, b_qkv, cos_np, sin_np, w_qkv, kc, vc)

        hid, qkv1 = pl.pallas_call(
            main_kernel,
            out_shape=(jax.ShapeDtypeStruct((SEQS, D), BF16), jax.ShapeDtypeStruct((SEQS, QKV), F32)),
            in_specs=[smem] + [vmem] * 11 + [hbm] * 6,
            out_specs=(vmem, vmem),
            scratch_shapes=[
                pltpu.VMEM((D, QKV), BF16), pltpu.VMEM((HEADS * HEAD, D), BF16), pltpu.VMEM((D, UP), BF16),
                pltpu.VMEM((FF, D), BF16)] + kv_buffers + [
                pltpu.VMEM((2, 3, ROWS, STAT), F32),
                pltpu.VMEM((4, 4, OWN, D), F32),
                pltpu.VMEM((4, 3, OWN, D), F32),
                pltpu.VMEM((3, 4, OWN, D), F32),
                pltpu.VMEM((OWN, D), F32),
                pltpu.VMEM((4, OWN, D), F32),
                pltpu.VMEM((ROWS, HEADS * HEAD), BF16),
                pltpu.VMEM((ROWS, CH), BF16),
                pltpu.VMEM((ROWS, UP), F32),
                pltpu.VMEM((ROWS, FF), BF16),
                pltpu.VMEM((4, ROWS, QKV), F32),
                pltpu.VMEM((SEQS, STAT), F32),
                pltpu.VMEM((4, 4, OWN, D), F32),
            ] + row8 + [
                dma((4, NCH)), dma((2,)), dma((2, 3)), dma((2, 3)), dma((4, 3, NCH)), dma((4, 3, NCH)),
                dma((3, 3, NCH)), dma((3, 3, NCH)), dma((3,)), dma((3,)), dma((4, 4)), dma((4, 4))],
            compiler_params=pltpu.CompilerParams(vmem_limit_bytes=VMEM_MAX, collective_id=0, has_side_effects=True),
            name="main",
        )(positions, stats0, qkv0, cos_rows, sin_rows, hidden, ln_gain, ln_bias, b_qkv, b_dense, b_up, b_down,
          w_qkv, w_dense, w_up, w_down, kc, vc)

        hidden_out, ko, vo = pl.pallas_call(
            exit_kernel,
            out_shape=(jax.ShapeDtypeStruct((SEQS, D), BF16), cache, cache),
            in_specs=[smem, vmem, vmem] + [hbm] * 4,
            out_specs=(vmem, hbm, hbm),
            scratch_shapes=kv_buffers + [dma((NGRP,))] * 4,
            input_output_aliases={5: 1, 6: 2},
            compiler_params=pltpu.CompilerParams(vmem_limit_bytes=VMEM_MAX),
            name="exit",
        )(positions, qkv1, hid, kc, vc, ko, vo)
        return hidden_out, ko.reshape(k_cache.shape), vo.reshape(v_cache.shape)

    return jax.shard_map(device_step, mesh=mesh, in_specs=in_specs, out_specs=out_specs, check_vma=False)
```

```python
import functools

import jax
import jax.numpy as jnp
import numpy as np
from jax import lax
from jax.experimental import pallas as pl
from jax.experimental.pallas import tpu as pltpu
from jax.sharding import PartitionSpec as P

MESH = pl.DeviceIdType.MESH
F32 = jnp.float32
BF16 = jnp.bfloat16
BLOCK_SIZE = 64
LOCAL_BLOCKS = 16
VERT_STRIDE = 8
ROPE_THETA = 1000000.0
GELU_LIMIT = 20.0
NORM_EPS = 0.00001
MASKED = -1e30

SEQS = 64
ROWS = 16
OWN = 8
SEQ_LEN = 512
SLOTS = 128
D = 3072
HEAD = 128
KV = 2
GROUP = 3
HEADS = KV * GROUP
QKV = 1280
QW = HEADS * HEAD
KVW = 2 * KV * HEAD
UP = 4096
FF = 2048
STAT = HEADS * HEAD + HEAD
NCH = 3
CH = D // NCH
GRP = 8
NGRP = SEQS // GRP
VMEM_MAX = 67043328


def rope_table():
    half = HEAD // 2
    inv = (ROPE_THETA ** (-np.arange(half).astype(np.float32) * np.float32(2.0 / HEAD))).astype(np.float32)
    angle = (np.arange(SEQ_LEN).astype(np.float32)[:, None] * inv[None, :]).astype(np.float64)
    cos, sin = np.cos(angle).astype(np.float32), np.sin(angle).astype(np.float32)
    return np.concatenate([cos, sin], 1)


def norm_rows(wide, gain, shift):
    mean = jnp.mean(wide, axis=-1, keepdims=True)
    centred = wide - mean
    var = jnp.mean(centred * centred, axis=-1, keepdims=True)
    return (centred * lax.rsqrt(var + NORM_EPS) * gain + shift).astype(BF16)


def param_row(ref, layer, which=None):
    rows = ref[...] if which is None else ref[layer]
    pick = layer if which is None else which
    return rows.astype(F32)[pick:pick + 1]


def round_bf16(x):
    return x.astype(BF16).astype(F32)


def dot(a, b):
    return jnp.dot(a, b, preferred_element_type=F32)


def turn_columns(acc, q_ref, kv_ref, cos, sin):
    for c in range(KV):
        for g in range(GROUP + 2):
            x = acc[:, (c * 5 + g) * HEAD:(c * 5 + g + 1) * HEAD]
            if g <= GROUP:
                x = x * cos + pltpu.roll(x, HEAD // 2, 1) * sin
            x = round_bf16(x)
            if g < GROUP:
                q_ref[:, (c * GROUP + g) * HEAD:(c * GROUP + g + 1) * HEAD] = x
            else:
                at = (c * 2 + g - GROUP) * HEAD
                kv_ref[:, at:at + HEAD] = x


def attend(sparse, pos_ref, q8, kbuf, vbuf, s8, acc8, ml8):
    t, s = lax.axis_index("tp"), lax.axis_index("sp")
    row = lax.broadcasted_iota(jnp.int32, (8, KV * SLOTS), 0)
    col = lax.broadcasted_iota(jnp.int32, (8, KV * SLOTS), 1)
    slot = s * SLOTS + col // KV
    same = (col % KV) == row // GROUP
    vertical = (slot // BLOCK_SIZE + (t * HEADS + row) + 1) % VERT_STRIDE == 0
    for b in range(SEQS):
        at = slice(b * 8, b * 8 + 8)
        p = pos_ref[b]
        scores = lax.dot_general(q8[at, :].astype(BF16), kbuf[b], (((1,), (1,)), ((), ())), preferred_element_type=F32)
        keep = (slot < p) & same
        if sparse:
            near = (p // BLOCK_SIZE - slot // BLOCK_SIZE) < LOCAL_BLOCKS
            keep = keep & (near | vertical)
        s8[at, :] = jnp.where(keep, scores * (1.0 / HEAD), -jnp.inf)
    for r in range(8):
        at = slice(r * SEQS, (r + 1) * SEQS)
        scores = s8[at, :]
        peak = jnp.maximum(jnp.max(scores, axis=-1, keepdims=True), MASKED)
        weights = jnp.exp(scores - peak)
        s8[at, :] = weights
        total = jnp.sum(weights, axis=-1, keepdims=True)
        low = lax.broadcasted_iota(jnp.int32, (SEQS, HEAD), 1) < HEADS
        ml8[at, :] = jnp.where(low, peak, total)
    for b in range(SEQS):
        at = slice(b * 8, b * 8 + 8)
        acc8[at, :] = dot(s8[at, :].astype(BF16), vbuf[b])


def pack_stats(stats, acc8, ml8):
    lane = lax.broadcasted_iota(jnp.int32, (SEQS, HEAD), 1)
    tail = jnp.zeros((SEQS, HEAD), F32)
    for h in range(HEADS):
        at = pl.ds(h, SEQS, stride=8)
        stats[:, h * HEAD:(h + 1) * HEAD] = acc8[at, :]
        tail = jnp.where((lane == h) | (lane == HEADS + h), ml8[at, :], tail)
    stats[:, HEADS * HEAD:] = tail


def put_new_rows(group, pos_ref, kv_ref, kbuf, vbuf):
    s = lax.axis_index("sp")
    row = lax.broadcasted_iota(jnp.int32, (16, HEAD), 0)
    fresh_rows = kv_ref[pl.ds(pl.multiple_of(group * GRP, GRP), GRP), :]
    for j in range(GRP):
        b = group * GRP + j
        local = pos_ref[b] - s * SLOTS
        inside = jnp.where((local >= 0) & (local < SLOTS), 1, 0)
        local = jnp.clip(local, 0, SLOTS - 1)
        at = pl.ds(pl.multiple_of((local // 8) * 16, 16), 16)
        target = jnp.where(inside == 1, local % 8, 99)
        hit = (row // KV) == target
        for i, buf in enumerate((kbuf, vbuf)):
            first, second = (fresh_rows[j:j + 1, (2 * c + i) * HEAD:(2 * c + i + 1) * HEAD] for c in range(KV))
            fresh = jnp.where(row % KV == 0, first, second)
            buf[b, at, :] = jnp.where(hit, fresh, buf[b, at, :].astype(F32)).astype(BF16)


def exit_kernel(pos_ref, kv0, kv1, hid, kc_hbm, vc_hbm, hid_out, ko_hbm, vo_hbm, kbuf, vbuf, sems):
    def copies(layer, g, out):
        at = pl.ds(g * GRP, GRP)
        pairs = ((kc_hbm, kbuf, ko_hbm), (vc_hbm, vbuf, vo_hbm))
        return [pltpu.make_async_copy(buf.at[layer, at] if out else src.at[layer, at],
                                      dst.at[layer, at] if out else buf.at[layer, at], sems.at[i + 2 * out, layer, g])
                for i, (src, buf, dst) in enumerate(pairs)]

    for layer in range(2):
        for g in range(NGRP):
            for copy in copies(layer, g, 0):
                copy.start()
    hid_out[...] = hid[...]
    for layer, kv in enumerate((kv0, kv1)):
        def one_group(g, carry, layer=layer, kv=kv):
            for copy in copies(layer, g, 0):
                copy.wait()
            put_new_rows(g, pos_ref, kv, kbuf.at[layer], vbuf.at[layer])
            for copy in copies(layer, g, 1):
                copy.start()
            return carry

        lax.fori_loop(0, NGRP, one_group, 0)
    for layer in range(2):
        def drain(g, carry, layer=layer):
            for copy in copies(layer, g, 1):
                copy.wait()
            return carry

        lax.fori_loop(0, NGRP, drain, 0)


def main_kernel(pos_ref, hidden, gain, shift, b_qkv, b_dense, b_up, b_down, table,
                wqkv_hbm, wdense_hbm, wup_hbm, wdown_hbm, kc_hbm, vc_hbm,
                hid, kv0, kv1_out,
                wqkv, wdense, wup, wdown, kbuf, vbuf,
                mix, part, summed, spread, x_own, o16, u16, h_s, m16, u_s, acc, q0, q1, kv1, stats0, stats1, fin,
                cos_rows, sin_rows, q8, s8, acc8, ml8,
                w_sem, kv_sem, mix_send, mix_recv, part_send, part_recv, spread_send, spread_recv,
                q_send, q_recv, fin_send, fin_recv, z_send):
    t, s = lax.axis_index("tp"), lax.axis_index("sp")
    owner = (t == 1) | (t == 2)
    half = jnp.clip(t - 1, 0, 1)
    unsent = {}

    def remote(src, dst, send_sem, recv_sem, axis, peer):
        return pltpu.make_async_remote_copy(src_ref=src, dst_ref=dst, send_sem=send_sem, recv_sem=recv_sem,
                                            device_id={axis: peer}, device_id_type=MESH)

    def send(*args, when=None, key=None):
        def go():
            remote(*args).start()

        def done():
            remote(*args).wait_send()

        if when is None:
            go()
        else:
            pl.when(when)(go)
        unsent.setdefault(key, []).append((done, when))

    def flush(key):
        for done, when in unsent.pop(key):
            if when is None:
                done()
            else:
                pl.when(when)(done)

    def arrived(*args):
        remote(*args).wait_recv()

    barrier = pltpu.get_barrier_semaphore()
    for axis, me in (("tp", t), ("sp", s)):
        for d in range(1, 4):
            pl.semaphore_signal(barrier, inc=1, device_id={axis: lax.rem(me + d, 4)}, device_id_type=MESH)

    cols = [pl.ds(n * CH, CH) for n in range(NCH)]

    def dense_copy(layer, n):
        return pltpu.make_async_copy(wdense_hbm.at[layer, :, cols[n]], wdense.at[:, cols[n]], w_sem.at[0, n])

    def up_copy(layer, n):
        return pltpu.make_async_copy(wup_hbm.at[layer, cols[n]], wup.at[cols[n]], w_sem.at[1, n])

    def down_copy(layer, n):
        return pltpu.make_async_copy(wdown_hbm.at[layer, :, cols[n]], wdown.at[:, cols[n]], w_sem.at[2, n])

    def qkv_copy(layer, n):
        return pltpu.make_async_copy(wqkv_hbm.at[layer, cols[n]], wqkv.at[cols[n]], w_sem.at[3, n])

    def k_copy(layer):
        return pltpu.make_async_copy(kc_hbm.at[layer], kbuf, kv_sem.at[0])

    def v_copy(layer):
        return pltpu.make_async_copy(vc_hbm.at[layer], vbuf, kv_sem.at[1])

    for n in range(NCH):
        qkv_copy(0, n).start()
    k_copy(0).start()
    v_copy(0).start()
    for copy_of in (dense_copy, up_copy, down_copy):
        for n in range(NCH):
            copy_of(0, n).start()

    my_rows = pl.ds(pl.multiple_of(s * ROWS, ROWS), ROWS)

    def pick_row(b, carry):
        p = pos_ref[b]
        cos_rows[pl.ds(b, 1), :] = table[pl.ds(p, 1), :]
        return carry

    lax.fori_loop(0, SEQS, pick_row, 0)
    both = cos_rows[...]
    other = pltpu.roll(both, HEAD // 2, 1)
    low = lax.broadcasted_iota(jnp.int32, (SEQS, HEAD), 1) < HEAD // 2
    cos_rows[...] = jnp.where(low, both, other)
    sin_rows[...] = jnp.where(low, -other, both)
    q8[...] = jnp.zeros_like(q8)
    u_s[...] = norm_rows(hidden[...].astype(F32), param_row(gain, 0, 0), param_row(shift, 0, 0))
    wide = hidden[my_rows, :].astype(F32)
    x_own[...] = jnp.where(half == 0, wide[:OWN], wide[OWN:])
    for n in range(NCH):
        qkv_copy(0, n).wait()
        piece = dot(u_s[:, n * CH:(n + 1) * CH], wqkv[n * CH:(n + 1) * CH, :])
        acc[...] = piece + param_row(b_qkv, 0) if n == 0 else acc[...] + piece
        qkv_copy(1, n).start()
    turn_columns(acc, q0, kv0, cos_rows[...], sin_rows[...])
    for h in range(HEADS):
        q8[pl.ds(h, SEQS, stride=8), :] = q0[:, h * HEAD:(h + 1) * HEAD]
    k_copy(0).wait()
    v_copy(0).wait()
    attend(True, pos_ref, q8, kbuf, vbuf, s8, acc8, ml8)
    k_copy(1).start()
    v_copy(1).start()
    pack_stats(stats0, acc8, ml8)
    pl.semaphore_wait(barrier, 6)

    def exchange(layer, stats):
        for d in (2, 1, 3):
            peer = lax.rem(s + d, 4)
            rows = pl.ds(pl.multiple_of(peer * ROWS, ROWS), ROWS)
            send(stats.at[rows], mix.at[layer, d - 1], mix_send.at[layer, d - 1], mix_recv.at[layer, d - 1], "sp", peer)

    def combine(layer, stats, q_rows, kv_rows):
        for d in range(1, 4):
            arrived(mix.at[layer, d - 1], mix.at[layer, d - 1], mix_send.at[layer, d - 1], mix_recv.at[layer, d - 1],
                    "sp", lax.rem(s + d, 4))
        shards = [stats[my_rows, :]] + [mix[layer, d] for d in range(3)]
        for h in range(HEADS):
            c = h // GROUP
            q = q_rows[:, h * HEAD:(h + 1) * HEAD]
            k = kv_rows[:, 2 * c * HEAD:(2 * c + 1) * HEAD]
            v = kv_rows[:, (2 * c + 1) * HEAD:(2 * c + 2) * HEAD]
            fresh = jnp.sum(q * k, axis=-1, keepdims=True) * (1.0 / HEAD)
            peaks = [x[:, QW + h:QW + h + 1] for x in shards]
            top = fresh
            for peak in peaks:
                top = jnp.maximum(top, peak)
            scale = jnp.exp(fresh - top)
            num, den = v * scale, scale
            for x, peak in zip(shards, peaks):
                scale = jnp.exp(peak - top)
                num = num + x[:, h * HEAD:(h + 1) * HEAD] * scale
                den = den + x[:, QW + HEADS + h:QW + HEADS + h + 1] * scale
            o16[:, h * HEAD:(h + 1) * HEAD] = (num / den).astype(BF16)

    def reduce_rows(phase, lhs, weights, layer, copy_of, reload):
        turn = phase % 2
        if phase >= 2:
            flush(("part", phase - 2))
        for n in range(NCH):
            copy_of(layer, n).wait()
            piece = dot(lhs[...], weights[:, n * CH:(n + 1) * CH])
            for i in range(2):
                part[turn, i, :, n * CH:(n + 1) * CH] = piece[OWN * i:OWN * (i + 1)]
                slot = jnp.clip(lax.rem(t - (i + 1) + 4, 4) - 1, 0, 2)
                send(part.at[turn, i, :, cols[n]], summed.at[turn, slot, :, cols[n]],
                     part_send.at[phase, i, n], part_recv.at[phase, slot, n], "tp", i + 1, when=t != i + 1,
                     key=("part", phase))
            if reload:
                copy_of(layer + 1, n).start()

    def sum_rows(phase, n):
        turn = phase % 2
        for d in range(3):
            dst = summed.at[turn, d, :, cols[n]]
            arrived(dst, dst, part_send.at[phase, 0, n], part_recv.at[phase, d, n], "tp", lax.rem(t + 1, 4))
        at = slice(n * CH, (n + 1) * CH)
        return part[turn, half, :, at] + summed[turn, 0, :, at] + summed[turn, 1, :, at] + summed[turn, 2, :, at]

    def add_rows(phase, bias):
        for n in range(NCH):
            at = slice(n * CH, (n + 1) * CH)
            x_own[:, at] = round_bf16(x_own[:, at] + sum_rows(phase, n) + bias[:, at])

    def spread_rows(phase, layer, which):
        rows = norm_rows(x_own[...], param_row(gain, layer, which), param_row(shift, layer, which))
        spread[phase % 2, half] = rows.astype(F32)

    def send_rows(phase):
        for n in range(NCH):
            for d in range(1, 4):
                block = spread.at[phase % 2, half, :, cols[n]]
                send(block, block, spread_send.at[phase, d - 1, n], spread_recv.at[phase, half, n], "tp",
                     lax.rem(t + d, 4), when=owner, key=("spread", phase))

    def take_rows(phase, n):
        for i in range(2):
            @pl.when(t != i + 1)
            def _():
                dst = spread.at[phase % 2, i, :, cols[n]]
                arrived(dst, dst, spread_send.at[phase, 0, n], spread_recv.at[phase, i, n], "tp", lax.rem(t + 1, 4))
        at = slice(n * CH, (n + 1) * CH)
        u16[...] = jnp.concatenate([spread[phase % 2, 0, :, at], spread[phase % 2, 1, :, at]], axis=0).astype(BF16)

    lane = lax.broadcasted_iota(jnp.int32, (ROWS, 1024), 1)
    pick = (lax.broadcasted_iota(jnp.int32, (256, 128), 0) == 2 * lax.broadcasted_iota(jnp.int32, (256, 128), 1))
    pick = jnp.where(pick, 1.0, 0.0).astype(BF16)

    def finish_layer(layer):
        last = layer == 1
        reduce_rows(2 * layer, o16, wdense, layer, dense_copy, not last)

        if last:
            flush(("spread", 0))

        @pl.when(owner)
        def _():
            add_rows(2 * layer, param_row(b_dense, layer))
            spread_rows(2 * layer, layer, 1)

        send_rows(2 * layer)
        bias = param_row(b_up, layer)
        for n in range(NCH):
            up_copy(layer, n).wait()
            take_rows(2 * layer, n)
            for c in range(4):
                at = slice(c * 1024, (c + 1) * 1024)
                piece = dot(u16[...], wup[n * CH:(n + 1) * CH, at])
                h_s[:, at] = piece + bias[:, at] if n == 0 else h_s[:, at] + piece
            if not last:
                up_copy(layer + 1, n).start()
        for c in range(4):
            pair = h_s[:, c * 1024:(c + 1) * 1024]
            gate = jnp.minimum(pair, GELU_LIMIT)
            line = jnp.clip(pltpu.roll(pair, 1023, 1), -GELU_LIMIT, GELU_LIMIT)
            act = gate * jax.nn.sigmoid(1.702 * gate) * (line + 1.0)
            act = jnp.where(lane % 2 == 0, act, 0.0).astype(BF16)
            for k in range(4):
                at = slice(c * 512 + k * 128, c * 512 + (k + 1) * 128)
                m16[:, at] = dot(act[:, k * 256:(k + 1) * 256], pick).astype(BF16)
        reduce_rows(2 * layer + 1, m16, wdown, layer, down_copy, not last)

    exchange(0, stats0)
    combine(0, stats0, q0[my_rows, :], kv0[my_rows, :])
    finish_layer(0)

    @pl.when(owner)
    def _():
        add_rows(1, param_row(b_down, 0))
        spread_rows(1, 1, 0)

    send_rows(1)
    some = acc.at[pl.ds(0, ROWS)]
    for n in range(NCH):
        qkv_copy(1, n).wait()
        take_rows(1, n)
        piece = dot(u16[...], wqkv[n * CH:(n + 1) * CH, :])
        some[...] = piece + param_row(b_qkv, 1) if n == 0 else some[...] + piece
    turn_columns(some, q1.at[s], kv1.at[s], cos_rows[my_rows, :], sin_rows[my_rows, :])
    for i, ref in enumerate((q1, kv1)):
        for d in (2, 1, 3):
            send(ref.at[s], ref.at[s], q_send.at[i, d - 1], q_recv.at[i, d - 1], "sp", lax.rem(s + d, 4))

    def gathered(i, ref):
        for d in range(1, 4):
            dst = ref.at[lax.rem(s - d + 4, 4)]
            arrived(dst, dst, q_send.at[i, d - 1], q_recv.at[i, d - 1], "sp", lax.rem(s + d, 4))

    gathered(0, q1)
    for i in range(4):
        for h in range(HEADS):
            q8[pl.ds(i * ROWS * 8 + h, ROWS, stride=8), :] = q1[i, :, h * HEAD:(h + 1) * HEAD]
    k_copy(1).wait()
    v_copy(1).wait()
    attend(False, pos_ref, q8, kbuf, vbuf, s8, acc8, ml8)
    pack_stats(stats1, acc8, ml8)
    exchange(1, stats1)
    combine(1, stats1, q1[s], kv1[s])
    finish_layer(1)

    twin = s + 1 - 2 * lax.rem(s, 2)
    across = lax.rem(s + 2, 4)
    diagonal = lax.rem(twin + 2, 4)

    def hop(kind, block, i, n, axis, peer):
        return block, block, fin_send.at[kind, i, n], fin_recv.at[kind, i, n], axis, peer

    for n in range(NCH):
        at = slice(n * CH, (n + 1) * CH)
        bias = param_row(b_down, 1)[:, at]

        @pl.when(owner)
        def _():
            fin[s, half, :, at] = round_bf16(x_own[:, at] + sum_rows(3, n) + bias)

        mine = fin.at[s, half, :, cols[n]]
        for d in range(1, 4):
            send(mine, mine, z_send.at[d - 1, n], fin_recv.at[0, half, n], "tp", lax.rem(t + d, 4), when=owner)
        for i in range(2):
            block = fin.at[s, i, :, cols[n]]

            @pl.when(t != i + 1)
            def _():
                arrived(*hop(0, block, i, n, "tp", lax.rem(t + 1, 4)))

            send(*hop(1, block, i, n, "sp", across))
            send(*hop(2, block, i, n, "sp", twin))
    for n in range(NCH):
        for i in range(2):
            block = fin.at[across, i, :, cols[n]]
            arrived(*hop(1, block, i, n, "sp", across))
            send(*hop(3, block, i, n, "sp", twin))
    gathered(1, kv1)
    for i in range(4):
        kv1_out[i * ROWS:(i + 1) * ROWS, :] = kv1[i]
    for n in range(NCH):
        for i in range(2):
            arrived(*hop(2, fin.at[twin, i, :, cols[n]], i, n, "sp", twin))
            arrived(*hop(3, fin.at[diagonal, i, :, cols[n]], i, n, "sp", twin))
    for i in range(4):
        hid[i * ROWS:(i + 1) * ROWS, :] = jnp.concatenate([fin[i, 0], fin[i, 1]], axis=0).astype(BF16)
    for key in list(unsent):
        flush(key)


def solution(mesh):
    cache_spec = P(None, "dp", "sp", "tp", None)
    in_specs = (P("dp", None), P("dp"), cache_spec, cache_spec, P(), P(), P(None, None, "tp"), P(None, "tp"),
                P(None, "tp", None), P(), P(None, None, "tp"), P(None, "tp"), P(None, "tp", None), P())
    out_specs = (P("dp", None), cache_spec, cache_spec)
    table = rope_table()
    vmem, smem, hbm = (pl.BlockSpec(memory_space=m) for m in (pltpu.VMEM, pltpu.SMEM, pl.ANY))
    dma = pltpu.SemaphoreType.DMA

    def device_step(hidden, positions, k_cache, v_cache, ln_gain, ln_bias, w_qkv, b_qkv, w_dense, b_dense,
                    w_up, b_up, w_down, b_down):
        flat = (2, SEQS, SLOTS * KV, HEAD)
        kc, vc = k_cache.reshape(flat), v_cache.reshape(flat)
        cache = jax.ShapeDtypeStruct(flat, BF16)
        row8 = [pltpu.VMEM((SEQS * 8, n * HEAD), F32) for n in (1, 2, 1, 1)]
        fresh = jax.ShapeDtypeStruct((SEQS, KVW), F32)
        hid, kv0, kv1 = pl.pallas_call(
            main_kernel,
            out_shape=(jax.ShapeDtypeStruct((SEQS, D), BF16), fresh, fresh),
            in_specs=[smem] + [vmem] * 8 + [hbm] * 6,
            out_specs=(vmem, vmem, vmem),
            scratch_shapes=[
                pltpu.VMEM((D, QKV), BF16), pltpu.VMEM((QW, D), BF16), pltpu.VMEM((D, UP), BF16),
                pltpu.VMEM((FF, D), BF16)] + [pltpu.VMEM(flat[1:], BF16)] * 2 + [
                pltpu.VMEM((2, 3, ROWS, STAT), F32),
                pltpu.VMEM((2, 2, OWN, D), F32),
                pltpu.VMEM((2, 3, OWN, D), F32),
                pltpu.VMEM((2, 2, OWN, D), F32),
                pltpu.VMEM((OWN, D), F32),
                pltpu.VMEM((ROWS, QW), BF16),
                pltpu.VMEM((ROWS, CH), BF16),
                pltpu.VMEM((ROWS, UP), F32),
                pltpu.VMEM((ROWS, FF), BF16),
                pltpu.VMEM((SEQS, D), BF16),
                pltpu.VMEM((SEQS, QKV), F32),
                pltpu.VMEM((SEQS, QW), F32),
                pltpu.VMEM((4, ROWS, QW), F32),
                pltpu.VMEM((4, ROWS, KVW), F32),
                pltpu.VMEM((SEQS, STAT), F32),
                pltpu.VMEM((SEQS, STAT), F32),
                pltpu.VMEM((4, 2, OWN, D), F32),
                pltpu.VMEM((SEQS, HEAD), F32), pltpu.VMEM((SEQS, HEAD), F32),
            ] + row8 + [
                dma((4, NCH)), dma((2,)), dma((2, 3)), dma((2, 3)), dma((4, 2, NCH)), dma((4, 3, NCH)),
                dma((3, 3, NCH)), dma((3, 2, NCH)), dma((2, 3)), dma((2, 3)), dma((4, 2, NCH)), dma((4, 2, NCH)),
                dma((3, NCH))],
            compiler_params=pltpu.CompilerParams(vmem_limit_bytes=VMEM_MAX, collective_id=0, has_side_effects=True),
            name="main",
        )(positions, hidden, ln_gain, ln_bias, b_qkv, b_dense, b_up, b_down, table,
          w_qkv, w_dense, w_up, w_down, kc, vc)

        hidden_out, ko, vo = pl.pallas_call(
            exit_kernel,
            out_shape=(jax.ShapeDtypeStruct((SEQS, D), BF16), cache, cache),
            in_specs=[smem, vmem, vmem, vmem, hbm, hbm],
            out_specs=(vmem, hbm, hbm),
            scratch_shapes=[pltpu.VMEM(flat, BF16)] * 2 + [dma((4, 2, NGRP))],
            compiler_params=pltpu.CompilerParams(vmem_limit_bytes=VMEM_MAX),
            name="exit",
        )(positions, kv0, kv1, hid, kc, vc)
        return hidden_out, ko.reshape(k_cache.shape), vo.reshape(v_cache.shape)

    return jax.shard_map(device_step, mesh=mesh, in_specs=in_specs, out_specs=out_specs, check_vma=False)
```

```python
import functools

import jax
import jax.numpy as jnp
import numpy as np
from jax import lax
from jax.experimental import pallas as pl
from jax.experimental.pallas import tpu as pltpu
from jax.sharding import PartitionSpec as P

MESH = pl.DeviceIdType.MESH
F32 = jnp.float32
BF16 = jnp.bfloat16
BLOCK_SIZE = 64
LOCAL_BLOCKS = 16
VERT_STRIDE = 8
ROPE_THETA = 1000000.0
GELU_LIMIT = 20.0
NORM_EPS = 0.00001
MASKED = -1e30

SEQS = 64
ROWS = 16
OWN = 4
SEQ_LEN = 512
SLOTS = 128
D = 3072
HEAD = 128
KV = 2
GROUP = 3
HEADS = KV * GROUP
QKV = 1280
QW = HEADS * HEAD
KVW = 2 * KV * HEAD
UP = 4096
FF = 2048
STAT = HEADS * HEAD + HEAD
NCH = 4
CH = D // NCH
GRP = 8
NGRP = SEQS // GRP
VMEM_MAX = 67043328


def rope_table():
    half = HEAD // 2
    inv = (ROPE_THETA ** (-np.arange(half).astype(np.float32) * np.float32(2.0 / HEAD))).astype(np.float32)
    angle = (np.arange(SEQ_LEN).astype(np.float32)[:, None] * inv[None, :]).astype(np.float64)
    cos, sin = np.cos(angle).astype(np.float32), np.sin(angle).astype(np.float32)
    return np.concatenate([cos, sin], 1)


def norm_rows(wide, gain, shift):
    mean = jnp.mean(wide, axis=-1, keepdims=True)
    centred = wide - mean
    var = jnp.mean(centred * centred, axis=-1, keepdims=True)
    return (centred * lax.rsqrt(var + NORM_EPS) * gain + shift).astype(BF16)


def param_row(ref, layer, which=None):
    rows = ref[...] if which is None else ref[layer]
    pick = layer if which is None else which
    return rows.astype(F32)[pick:pick + 1]


def round_bf16(x):
    return x.astype(BF16).astype(F32)


def dot(a, b):
    return jnp.dot(a, b, preferred_element_type=F32)


def turn_columns(acc, q_ref, kv_ref, cos, sin):
    for c in range(KV):
        for g in range(GROUP + 2):
            x = acc[:, (c * 5 + g) * HEAD:(c * 5 + g + 1) * HEAD]
            if g <= GROUP:
                x = x * cos + pltpu.roll(x, HEAD // 2, 1) * sin
            x = round_bf16(x)
            if g < GROUP:
                q_ref[:, (c * GROUP + g) * HEAD:(c * GROUP + g + 1) * HEAD] = x
            else:
                at = (c * 2 + g - GROUP) * HEAD
                kv_ref[:, at:at + HEAD] = x


def attend(sparse, pos_ref, q8, kbuf, vbuf, s8, acc8, ml8):
    t, s = lax.axis_index("tp"), lax.axis_index("sp")
    row = lax.broadcasted_iota(jnp.int32, (8, KV * SLOTS), 0)
    col = lax.broadcasted_iota(jnp.int32, (8, KV * SLOTS), 1)
    slot = s * SLOTS + col // KV
    same = (col % KV) == row // GROUP
    vertical = (slot // BLOCK_SIZE + (t * HEADS + row) + 1) % VERT_STRIDE == 0
    for b in range(SEQS):
        at = slice(b * 8, b * 8 + 8)
        p = pos_ref[b]
        scores = lax.dot_general(q8[at, :].astype(BF16), kbuf[b], (((1,), (1,)), ((), ())), preferred_element_type=F32)
        keep = (slot < p) & same
        if sparse:
            near = (p // BLOCK_SIZE - slot // BLOCK_SIZE) < LOCAL_BLOCKS
            keep = keep & (near | vertical)
        s8[at, :] = jnp.where(keep, scores * (1.0 / HEAD), -jnp.inf)
    for r in range(8):
        at = slice(r * SEQS, (r + 1) * SEQS)
        scores = s8[at, :]
        peak = jnp.maximum(jnp.max(scores, axis=-1, keepdims=True), MASKED)
        weights = jnp.exp(scores - peak)
        s8[at, :] = weights
        total = jnp.sum(weights, axis=-1, keepdims=True)
        low = lax.broadcasted_iota(jnp.int32, (SEQS, HEAD), 1) < HEADS
        ml8[at, :] = jnp.where(low, peak, total)
    for b in range(SEQS):
        at = slice(b * 8, b * 8 + 8)
        acc8[at, :] = dot(s8[at, :].astype(BF16), vbuf[b])


def pack_stats(stats, acc8, ml8):
    lane = lax.broadcasted_iota(jnp.int32, (SEQS, HEAD), 1)
    tail = jnp.zeros((SEQS, HEAD), F32)
    for h in range(HEADS):
        at = pl.ds(h, SEQS, stride=8)
        stats[:, h * HEAD:(h + 1) * HEAD] = acc8[at, :]
        tail = jnp.where((lane == h) | (lane == HEADS + h), ml8[at, :], tail)
    stats[:, HEADS * HEAD:] = tail


def put_new_rows(group, pos_ref, kv_ref, kbuf, vbuf):
    s = lax.axis_index("sp")
    row = lax.broadcasted_iota(jnp.int32, (16, HEAD), 0)
    fresh_rows = kv_ref[pl.ds(pl.multiple_of(group * GRP, GRP), GRP), :]
    for j in range(GRP):
        b = group * GRP + j
        local = pos_ref[b] - s * SLOTS
        inside = jnp.where((local >= 0) & (local < SLOTS), 1, 0)
        local = jnp.clip(local, 0, SLOTS - 1)
        at = pl.ds(pl.multiple_of((local // 8) * 16, 16), 16)
        target = jnp.where(inside == 1, local % 8, 99)
        hit = (row // KV) == target
        for i, buf in enumerate((kbuf, vbuf)):
            first, second = (fresh_rows[j:j + 1, (2 * c + i) * HEAD:(2 * c + i + 1) * HEAD] for c in range(KV))
            fresh = jnp.where(row % KV == 0, first, second)
            buf[b, at, :] = jnp.where(hit, fresh, buf[b, at, :].astype(F32)).astype(BF16)


def stream_cache(layer, src_pair, buf_pair, dst_pair, sems):
    def copies(g, out):
        at = pl.ds(g * GRP, GRP)
        if out:
            return [pltpu.make_async_copy(buf.at[at], dst.at[layer, at], sems.at[2 + i, g])
                    for i, (buf, dst) in enumerate(zip(buf_pair, dst_pair))]
        return [pltpu.make_async_copy(src.at[layer, at], buf.at[at], sems.at[i, g])
                for i, (src, buf) in enumerate(zip(src_pair, buf_pair))]

    return copies


def store_cache(copies, pos_ref, kv_ref, kbuf, vbuf):
    def one_group(g, carry):
        for copy in copies(g, 0):
            copy.wait()
        put_new_rows(g, pos_ref, kv_ref, kbuf, vbuf)
        for copy in copies(g, 1):
            copy.start()
        return carry

    lax.fori_loop(0, NGRP, one_group, 0)


def drain_cache(copies):
    def drain(g, carry):
        for copy in copies(g, 1):
            copy.wait()
        return carry

    lax.fori_loop(0, NGRP, drain, 0)


def fetch(sources, targets, sems):
    copies = [pltpu.make_async_copy(src, dst, sems.at[i]) for i, (src, dst) in enumerate(zip(sources, targets))]
    for copy in copies:
        copy.start()
    return copies


def entry_kernel(pos_hbm, hidden_hbm, gain_hbm, shift_hbm, b_hbm, table_hbm, w_hbm, kc_hbm, vc_hbm,
                 ko_hbm, vo_hbm, q0_hbm, kv0_hbm, stats0_hbm, cos_hbm, sin_hbm,
                 pos_ref, hidden, gain, shift, b_qkv, table, q0, kv0, stats0, cos_rows, sin_rows,
                 wbuf, kbuf, vbuf, u_s, acc, q8, s8, acc8, ml8, w_sem, sems, small):
    first = fetch((pos_hbm, hidden_hbm, gain_hbm, shift_hbm, b_hbm, table_hbm),
                  (pos_ref, hidden, gain, shift, b_qkv, table), small)
    copies = stream_cache(0, (kc_hbm, vc_hbm), (kbuf, vbuf), (ko_hbm, vo_hbm), sems)

    def w_copy(n):
        return pltpu.make_async_copy(w_hbm.at[0, pl.ds(n * CH, CH)], wbuf.at[pl.ds(n * CH, CH)], w_sem.at[n])

    for n in range(NCH):
        w_copy(n).start()

    q8[...] = jnp.zeros_like(q8)
    for copy in first:
        copy.wait()

    def pick_row(b, carry):
        p = pos_ref[b]
        cos_rows[pl.ds(b, 1), :] = table[pl.ds(p, 1), :]
        return carry

    lax.fori_loop(0, SEQS, pick_row, 0)
    both = cos_rows[...]
    other = pltpu.roll(both, HEAD // 2, 1)
    low = lax.broadcasted_iota(jnp.int32, (SEQS, HEAD), 1) < HEAD // 2
    cos_rows[...] = jnp.where(low, both, other)
    sin_rows[...] = jnp.where(low, -other, both)
    u_s[...] = norm_rows(hidden[...].astype(F32), param_row(gain, 0, 0), param_row(shift, 0, 0))
    for n in range(NCH):
        w_copy(n).wait()
        if n == 0:
            for g in range(NGRP):
                for copy in copies(g, 0):
                    copy.start()
        piece = dot(u_s[:, n * CH:(n + 1) * CH], wbuf[n * CH:(n + 1) * CH, :])
        acc[...] = piece + param_row(b_qkv, 0) if n == 0 else acc[...] + piece
    turn_columns(acc, q0, kv0, cos_rows[...], sin_rows[...])
    outs = fetch((q0, kv0, cos_rows, sin_rows), (q0_hbm, kv0_hbm, cos_hbm, sin_hbm), small)
    for h in range(HEADS):
        q8[pl.ds(h, SEQS, stride=8), :] = q0[:, h * HEAD:(h + 1) * HEAD]
    store_cache(copies, pos_ref, kv0, kbuf, vbuf)
    attend(True, pos_ref, q8, kbuf, vbuf, s8, acc8, ml8)
    pack_stats(stats0, acc8, ml8)
    stats_out = pltpu.make_async_copy(stats0, stats0_hbm, small.at[4])
    stats_out.start()
    drain_cache(copies)
    for copy in outs + [stats_out]:
        copy.wait()


def exit_kernel(pos_hbm, kv_hbm, hid_hbm, kc_hbm, vc_hbm, ka_hbm, va_hbm, hid_out, ko_hbm, vo_hbm,
                kbuf, vbuf, kv, hid, pos_ref, sems, small):
    copies = stream_cache(1, (kc_hbm, vc_hbm), (kbuf, vbuf), (ko_hbm, vo_hbm), sems)
    first = [pltpu.make_async_copy(src, dst, small.at[i])
             for i, (src, dst) in enumerate(((pos_hbm, pos_ref), (kv_hbm, kv), (hid_hbm, hid)))]
    hid_back = pltpu.make_async_copy(hid, hid_out, small.at[3])
    for copy in first:
        copy.start()
    for g in range(NGRP):
        for copy in copies(g, 0):
            copy.start()
    for copy in first:
        copy.wait()
    hid_back.start()
    store_cache(copies, pos_ref, kv, kbuf, vbuf)
    drain_cache(copies)
    hid_back.wait()


def main_kernel(pos_hbm, q0_hbm, kv0_hbm, stats0_hbm, cos_hbm, sin_hbm, hidden_hbm,
                gain_hbm, shift_hbm, bqkv_hbm, bdense_hbm, bup_hbm, bdown_hbm,
                wqkv_hbm, wdense_hbm, wup_hbm, wdown_hbm, kc_hbm, vc_hbm,
                hid, kv1_out,
                pos_ref, q0, kv0, stats0, cos_rows, sin_rows, hidden, gain, shift, b_qkv, b_dense, b_up, b_down, small,
                wqkv, wdense, wup, wdown, kbuf, vbuf,
                mix, part, summed, spread, x_own, o16, u16, h_s, m16, acc, q1, kv1, stats1, fin, q8, s8, acc8, ml8,
                w_sem, kv_sem, mix_send, mix_recv, part_send, part_recv, spread_send, spread_recv,
                q_send, q_recv, fin_send, fin_recv, z_send):
    t, s = lax.axis_index("tp"), lax.axis_index("sp")
    far = (2, 1, 3)
    unsent = {}

    def remote(src, dst, send_sem, recv_sem, axis, peer):
        return pltpu.make_async_remote_copy(src_ref=src, dst_ref=dst, send_sem=send_sem, recv_sem=recv_sem,
                                            device_id={axis: peer}, device_id_type=MESH)

    def send(*args, key=None):
        copy = remote(*args)
        copy.start()
        unsent.setdefault(key, []).append(copy)

    def flush(key):
        for copy in unsent.pop(key):
            copy.wait_send()

    def arrived(*args):
        remote(*args).wait_recv()

    barrier = pltpu.get_barrier_semaphore()
    for axis, me in (("tp", t), ("sp", s)):
        for d in range(1, 4):
            pl.semaphore_signal(barrier, inc=1, device_id={axis: lax.rem(me + d, 4)}, device_id_type=MESH)

    my_rows = pl.ds(pl.multiple_of(s * ROWS, ROWS), ROWS)
    first = fetch((stats0_hbm, pos_hbm, q0_hbm.at[my_rows], kv0_hbm.at[my_rows], cos_hbm.at[my_rows],
                   sin_hbm.at[my_rows], hidden_hbm.at[my_rows], gain_hbm, shift_hbm, bqkv_hbm, bdense_hbm, bup_hbm,
                   bdown_hbm),
                  (stats0, pos_ref, q0, kv0, cos_rows, sin_rows, hidden, gain, shift, b_qkv, b_dense, b_up, b_down),
                  small)
    cols = [pl.ds(n * CH, CH) for n in range(NCH)]

    def dense_copy(layer, n):
        return pltpu.make_async_copy(wdense_hbm.at[layer, :, cols[n]], wdense.at[:, cols[n]], w_sem.at[0, n])

    def up_copy(layer, n):
        return pltpu.make_async_copy(wup_hbm.at[layer, cols[n]], wup.at[cols[n]], w_sem.at[1, n])

    def down_copy(layer, n):
        return pltpu.make_async_copy(wdown_hbm.at[layer, :, cols[n]], wdown.at[:, cols[n]], w_sem.at[2, n])

    def qkv_copy(layer, n):
        return pltpu.make_async_copy(wqkv_hbm.at[layer, cols[n]], wqkv.at[cols[n]], w_sem.at[3, n])

    def k_copy(layer):
        return pltpu.make_async_copy(kc_hbm.at[layer], kbuf, kv_sem.at[0])

    def v_copy(layer):
        return pltpu.make_async_copy(vc_hbm.at[layer], vbuf, kv_sem.at[1])

    q8[...] = jnp.zeros_like(q8)
    for copy in first:
        copy.wait()
    for n in range(NCH):
        dense_copy(0, n).start()
    for n in range(NCH):
        up_copy(0, n).start()
    wide = hidden[...].astype(F32)
    for j in range(4):
        fin[0, j] = wide[OWN * j:OWN * (j + 1)]
    x_own[...] = fin[0, t]
    pl.semaphore_wait(barrier, 6)

    def exchange(layer, stats):
        for d in far:
            peer = lax.rem(s + d, 4)
            rows = pl.ds(pl.multiple_of(peer * ROWS, ROWS), ROWS)
            send(stats.at[rows], mix.at[layer, d - 1], mix_send.at[layer, d - 1], mix_recv.at[layer, d - 1], "sp", peer)

    def combine(layer, stats, q_rows, kv_rows):
        for d in range(1, 4):
            arrived(mix.at[layer, d - 1], mix.at[layer, d - 1], mix_send.at[layer, d - 1], mix_recv.at[layer, d - 1],
                    "sp", lax.rem(s + d, 4))
        shards = [stats[my_rows, :]] + [mix[layer, d] for d in range(3)]
        for h in range(HEADS):
            c = h // GROUP
            q = q_rows[:, h * HEAD:(h + 1) * HEAD]
            k = kv_rows[:, 2 * c * HEAD:(2 * c + 1) * HEAD]
            v = kv_rows[:, (2 * c + 1) * HEAD:(2 * c + 2) * HEAD]
            fresh = jnp.sum(q * k, axis=-1, keepdims=True) * (1.0 / HEAD)
            peaks = [x[:, QW + h:QW + h + 1] for x in shards]
            top = fresh
            for peak in peaks:
                top = jnp.maximum(top, peak)
            scale = jnp.exp(fresh - top)
            num, den = v * scale, scale
            for x, peak in zip(shards, peaks):
                scale = jnp.exp(peak - top)
                num = num + x[:, h * HEAD:(h + 1) * HEAD] * scale
                den = den + x[:, QW + HEADS + h:QW + HEADS + h + 1] * scale
            o16[:, h * HEAD:(h + 1) * HEAD] = (num / den).astype(BF16)

    def reduce_rows(phase, lhs, weights, layer, copy_of):
        turn = phase % 2
        if phase >= 2:
            flush(("part", phase - 2))
        for n in range(NCH):
            copy_of(layer, n).wait()
            piece = dot(lhs[...], weights[:, n * CH:(n + 1) * CH])
            for j in range(4):
                part[turn, j, :, n * CH:(n + 1) * CH] = piece[OWN * j:OWN * (j + 1)]
            for d in far:
                peer = lax.rem(t + d, 4)
                send(part.at[turn, peer, :, cols[n]], summed.at[turn, d - 1, :, cols[n]],
                     part_send.at[phase, d - 1, n], part_recv.at[phase, d - 1, n], "tp", peer, key=("part", phase))

    def sum_rows(phase, n):
        turn = phase % 2
        for d in range(1, 4):
            dst = summed.at[turn, d - 1, :, cols[n]]
            arrived(dst, dst, part_send.at[phase, d - 1, n], part_recv.at[phase, d - 1, n], "tp", lax.rem(t + d, 4))
        at = slice(n * CH, (n + 1) * CH)
        return part[turn, t, :, at] + summed[turn, 0, :, at] + summed[turn, 1, :, at] + summed[turn, 2, :, at]

    def add_rows(phase, bias):
        for n in range(NCH):
            at = slice(n * CH, (n + 1) * CH)
            x_own[:, at] = round_bf16(x_own[:, at] + sum_rows(phase, n) + bias[:, at])

    def spread_rows(phase, layer, which):
        rows = norm_rows(x_own[...], param_row(gain, layer, which), param_row(shift, layer, which))
        spread[phase % 2, t] = rows.astype(F32)
        for n in range(NCH):
            block = spread.at[phase % 2, t, :, cols[n]]
            for d in far:
                send(block, block, spread_send.at[phase, d - 1, n], spread_recv.at[phase, d - 1, n], "tp",
                     lax.rem(t + d, 4), key=("spread", phase))

    def take_rows(phase, n):
        for d in range(1, 4):
            dst = spread.at[phase % 2, lax.rem(t - d + 4, 4), :, cols[n]]
            arrived(dst, dst, spread_send.at[phase, d - 1, n], spread_recv.at[phase, d - 1, n], "tp", lax.rem(t + d, 4))
        at = slice(n * CH, (n + 1) * CH)
        u16[...] = jnp.concatenate([spread[phase % 2, j, :, at] for j in range(4)], axis=0).astype(BF16)

    lane = lax.broadcasted_iota(jnp.int32, (ROWS, 1024), 1)
    pick = (lax.broadcasted_iota(jnp.int32, (256, 128), 0) == 2 * lax.broadcasted_iota(jnp.int32, (256, 128), 1))
    pick = jnp.where(pick, 1.0, 0.0).astype(BF16)

    def finish_layer(layer):
        last = layer == 1
        reduce_rows(2 * layer, o16, wdense, layer, dense_copy)

        if last:
            flush(("spread", 0))

        add_rows(2 * layer, param_row(b_dense, layer))
        spread_rows(2 * layer, layer, 1)
        bias = param_row(b_up, layer)
        for n in range(NCH):
            up_copy(layer, n).wait()
            take_rows(2 * layer, n)
            for c in range(4):
                at = slice(c * 1024, (c + 1) * 1024)
                piece = dot(u16[...], wup[n * CH:(n + 1) * CH, at])
                h_s[:, at] = piece + bias[:, at] if n == 0 else h_s[:, at] + piece
        if not last:
            for n in range(NCH):
                qkv_copy(1, n).start()
        for c in range(4):
            pair = h_s[:, c * 1024:(c + 1) * 1024]
            gate = jnp.minimum(pair, GELU_LIMIT)
            line = jnp.clip(pltpu.roll(pair, 1023, 1), -GELU_LIMIT, GELU_LIMIT)
            act = gate * jax.nn.sigmoid(1.702 * gate) * (line + 1.0)
            act = jnp.where(lane % 2 == 0, act, 0.0).astype(BF16)
            for k in range(4):
                at = slice(c * 512 + k * 128, c * 512 + (k + 1) * 128)
                m16[:, at] = dot(act[:, k * 256:(k + 1) * 256], pick).astype(BF16)
        reduce_rows(2 * layer + 1, m16, wdown, layer, down_copy)
        if not last:
            k_copy(1).start()
            v_copy(1).start()

    exchange(0, stats0)
    for n in range(NCH):
        down_copy(0, n).start()
    combine(0, stats0, q0[...], kv0[...])
    finish_layer(0)

    add_rows(1, param_row(b_down, 0))
    spread_rows(1, 1, 0)
    for n in range(NCH):
        qkv_copy(1, n).wait()
        take_rows(1, n)
        piece = dot(u16[...], wqkv[n * CH:(n + 1) * CH, :])
        acc[...] = piece + param_row(b_qkv, 1) if n == 0 else acc[...] + piece
    for n in range(NCH):
        dense_copy(1, n).start()
    for n in range(NCH):
        up_copy(1, n).start()
    turn_columns(acc, q1.at[s], kv1.at[s], cos_rows[...], sin_rows[...])
    for i, ref in enumerate((q1, kv1)):
        for d in far:
            send(ref.at[s], ref.at[s], q_send.at[i, d - 1], q_recv.at[i, d - 1], "sp", lax.rem(s + d, 4))

    def gathered(i, ref):
        for d in range(1, 4):
            dst = ref.at[lax.rem(s - d + 4, 4)]
            arrived(dst, dst, q_send.at[i, d - 1], q_recv.at[i, d - 1], "sp", lax.rem(s + d, 4))

    gathered(0, q1)
    for i in range(4):
        for h in range(HEADS):
            q8[pl.ds(i * ROWS * 8 + h, ROWS, stride=8), :] = q1[i, :, h * HEAD:(h + 1) * HEAD]
    k_copy(1).wait()
    v_copy(1).wait()
    attend(False, pos_ref, q8, kbuf, vbuf, s8, acc8, ml8)
    pack_stats(stats1, acc8, ml8)
    for n in range(NCH):
        down_copy(1, n).start()
    exchange(1, stats1)
    combine(1, stats1, q1[s], kv1[s])
    finish_layer(1)

    twin = s + 1 - 2 * lax.rem(s, 2)
    across = lax.rem(s + 2, 4)
    diagonal = lax.rem(twin + 2, 4)

    def hop(kind, block, i, n, axis, peer):
        return block, block, fin_send.at[kind, i, n], fin_recv.at[kind, i, n], axis, peer

    bias = param_row(b_down, 1)
    for n in range(NCH):
        at = slice(n * CH, (n + 1) * CH)
        fin[s, t, :, at] = round_bf16(x_own[:, at] + sum_rows(3, n) + bias[:, at])
        block = fin.at[s, t, :, cols[n]]
        for d in far:
            send(block, block, z_send.at[d - 1, n], fin_recv.at[0, d, n], "tp", lax.rem(t + d, 4))
        send(*hop(1, block, 0, n, "sp", across))
        send(*hop(2, block, 0, n, "sp", twin))
    for n in range(NCH):
        for d in (1, 3, 2):
            block = fin.at[s, lax.rem(t - d + 4, 4), :, cols[n]]
            arrived(*hop(0, block, d, n, "tp", lax.rem(t + d, 4)))
            send(*hop(1, block, d, n, "sp", across))
            send(*hop(2, block, d, n, "sp", twin))
    for n in range(NCH):
        for d in range(4):
            block = fin.at[across, lax.rem(t - d + 4, 4), :, cols[n]]
            arrived(*hop(1, block, d, n, "sp", across))
            send(*hop(3, block, d, n, "sp", twin))
    gathered(1, kv1)
    for i in range(4):
        kv1_out[i * ROWS:(i + 1) * ROWS, :] = kv1[i]
    for n in range(NCH):
        for d in range(4):
            arrived(*hop(2, fin.at[twin, lax.rem(t - d + 4, 4), :, cols[n]], d, n, "sp", twin))
            arrived(*hop(3, fin.at[diagonal, lax.rem(t - d + 4, 4), :, cols[n]], d, n, "sp", twin))
    for i in range(4):
        hid[i * ROWS:(i + 1) * ROWS, :] = jnp.concatenate([fin[i, j] for j in range(4)], axis=0).astype(BF16)
    for key in list(unsent):
        flush(key)


def solution(mesh):
    cache_spec = P(None, "dp", "sp", "tp", None)
    in_specs = (P("dp", None), P("dp"), cache_spec, cache_spec, P(), P(), P(None, None, "tp"), P(None, "tp"),
                P(None, "tp", None), P(), P(None, None, "tp"), P(None, "tp"), P(None, "tp", None), P())
    out_specs = (P("dp", None), cache_spec, cache_spec)
    table = rope_table()
    vmem, hbm = (pl.BlockSpec(memory_space=m) for m in (pltpu.VMEM, pl.ANY))
    dma = pltpu.SemaphoreType.DMA

    def device_step(hidden, positions, k_cache, v_cache, ln_gain, ln_bias, w_qkv, b_qkv, w_dense, b_dense,
                    w_up, b_up, w_down, b_down):
        flat = (2, SEQS, SLOTS * KV, HEAD)
        kc, vc = k_cache.reshape(flat), v_cache.reshape(flat)
        cache = jax.ShapeDtypeStruct(flat, BF16)
        row8 = [pltpu.VMEM((SEQS * 8, n * HEAD), F32) for n in (1, 2, 1, 1)]
        buffers = [pltpu.VMEM(flat[1:], BF16)] * 2
        rows = [jax.ShapeDtypeStruct((SEQS, n), F32) for n in (QW, KVW, STAT, HEAD, HEAD)]
        big = pltpu.CompilerParams(vmem_limit_bytes=VMEM_MAX)
        ko, vo, q0, kv0, stats0, cos_rows, sin_rows = pl.pallas_call(
            entry_kernel,
            out_shape=(cache, cache, *rows),
            in_specs=[hbm] * 9,
            out_specs=(hbm,) * 7,
            scratch_shapes=[pltpu.SMEM((SEQS,), jnp.int32), pltpu.VMEM((SEQS, D), BF16), pltpu.VMEM((2, 2, D), BF16),
                            pltpu.VMEM((2, 2, D), BF16), pltpu.VMEM((2, QKV), BF16), pltpu.VMEM((SEQ_LEN, HEAD), F32)]
            + [pltpu.VMEM(x.shape, F32) for x in rows] + [pltpu.VMEM((D, QKV), BF16)] + buffers
            + [pltpu.VMEM((SEQS, D), BF16), pltpu.VMEM((SEQS, QKV), F32)] + row8 + [dma((NCH,)), dma((4, NGRP)), dma((6,))],
            compiler_params=big,
            name="entry",
        )(positions, hidden, ln_gain, ln_bias, b_qkv, table, w_qkv, kc, vc)

        hid, kv1 = pl.pallas_call(
            main_kernel,
            out_shape=(jax.ShapeDtypeStruct((SEQS, D), BF16), rows[1]),
            in_specs=[hbm] * 19,
            out_specs=(vmem, vmem),
            scratch_shapes=[
                pltpu.SMEM((SEQS,), jnp.int32), pltpu.VMEM((ROWS, QW), F32), pltpu.VMEM((ROWS, KVW), F32),
                pltpu.VMEM((SEQS, STAT), F32), pltpu.VMEM((ROWS, HEAD), F32), pltpu.VMEM((ROWS, HEAD), F32),
                pltpu.VMEM((ROWS, D), BF16), pltpu.VMEM((2, 2, D), BF16), pltpu.VMEM((2, 2, D), BF16),
                pltpu.VMEM((2, QKV), BF16), pltpu.VMEM((2, D), BF16), pltpu.VMEM((2, UP), BF16),
                pltpu.VMEM((2, D), BF16), dma((13,)),
                pltpu.VMEM((D, QKV), BF16), pltpu.VMEM((QW, D), BF16), pltpu.VMEM((D, UP), BF16),
                pltpu.VMEM((FF, D), BF16)] + buffers + [
                pltpu.VMEM((2, 3, ROWS, STAT), F32),
                pltpu.VMEM((2, 4, OWN, D), F32),
                pltpu.VMEM((2, 3, OWN, D), F32),
                pltpu.VMEM((2, 4, OWN, D), F32),
                pltpu.VMEM((OWN, D), F32),
                pltpu.VMEM((ROWS, QW), BF16),
                pltpu.VMEM((ROWS, CH), BF16),
                pltpu.VMEM((ROWS, UP), F32),
                pltpu.VMEM((ROWS, FF), BF16),
                pltpu.VMEM((ROWS, QKV), F32),
                pltpu.VMEM((4, ROWS, QW), F32),
                pltpu.VMEM((4, ROWS, KVW), F32),
                pltpu.VMEM((SEQS, STAT), F32),
                pltpu.VMEM((4, 4, OWN, D), F32),
            ] + row8 + [
                dma((4, NCH)), dma((2,)), dma((2, 3)), dma((2, 3)), dma((4, 3, NCH)), dma((4, 3, NCH)),
                dma((3, 3, NCH)), dma((3, 3, NCH)), dma((2, 3)), dma((2, 3)), dma((4, 4, NCH)), dma((4, 4, NCH)),
                dma((3, NCH))],
            compiler_params=pltpu.CompilerParams(vmem_limit_bytes=VMEM_MAX, collective_id=0, has_side_effects=True),
            name="main",
        )(positions, q0, kv0, stats0, cos_rows, sin_rows, hidden, ln_gain, ln_bias, b_qkv, b_dense, b_up, b_down,
          w_qkv, w_dense, w_up, w_down, kc, vc)

        hidden_out, ko, vo = pl.pallas_call(
            exit_kernel,
            out_shape=(jax.ShapeDtypeStruct((SEQS, D), BF16), cache, cache),
            in_specs=[hbm] * 7,
            out_specs=(hbm, hbm, hbm),
            scratch_shapes=buffers + [pltpu.VMEM((SEQS, KVW), F32), pltpu.VMEM((SEQS, D), BF16),
                                      pltpu.SMEM((SEQS,), jnp.int32), dma((4, NGRP)), dma((4,))],
            input_output_aliases={5: 1, 6: 2},
            compiler_params=big,
            name="exit",
        )(positions, kv1, hid, kc, vc, ko, vo)
        return hidden_out, ko.reshape(k_cache.shape), vo.reshape(v_cache.shape)

    return jax.shard_map(device_step, mesh=mesh, in_specs=in_specs, out_specs=out_specs, check_vma=False)
```

```python
import functools

import jax
import jax.numpy as jnp
import numpy as np
from jax import lax
from jax.experimental import pallas as pl
from jax.experimental.pallas import tpu as pltpu
from jax.sharding import PartitionSpec as P

MESH = pl.DeviceIdType.MESH
F32 = jnp.float32
BF16 = jnp.bfloat16
BLOCK_SIZE = 64
LOCAL_BLOCKS = 16
VERT_STRIDE = 8
ROPE_THETA = 1000000.0
GELU_LIMIT = 20.0
NORM_EPS = 0.00001
MASKED = -1e30

SEQS = 64
ROWS = 16
OWN = 4
SEQ_LEN = 512
SLOTS = 128
D = 3072
HEAD = 128
KV = 2
GROUP = 3
HEADS = KV * GROUP
QKV = 1280
QW = HEADS * HEAD
KVW = 2 * KV * HEAD
UP = 4096
FF = 2048
STAT = HEADS * HEAD + HEAD
NCH = 4
CH = D // NCH
GRP = 8
NGRP = SEQS // GRP
VMEM_MAX = 67043328


def rope_table():
    half = HEAD // 2
    inv = (ROPE_THETA ** (-np.arange(half).astype(np.float32) * np.float32(2.0 / HEAD))).astype(np.float32)
    angle = (np.arange(SEQ_LEN).astype(np.float32)[:, None] * inv[None, :]).astype(np.float64)
    cos, sin = np.cos(angle).astype(np.float32), np.sin(angle).astype(np.float32)
    return np.concatenate([cos, sin], 1)


def norm_rows(wide, gain, shift):
    mean = jnp.mean(wide, axis=-1, keepdims=True)
    centred = wide - mean
    var = jnp.mean(centred * centred, axis=-1, keepdims=True)
    return (centred * lax.rsqrt(var + NORM_EPS) * gain + shift).astype(BF16)


def param_row(ref, layer, which=None):
    rows = ref[...] if which is None else ref[layer]
    pick = layer if which is None else which
    return rows.astype(F32)[pick:pick + 1]


def round_bf16(x):
    return x.astype(BF16).astype(F32)


def dot(a, b):
    return jnp.dot(a, b, preferred_element_type=F32)


def turn_columns(acc, q_ref, kv_ref, cos, sin):
    for c in range(KV):
        for g in range(GROUP + 2):
            x = acc[:, (c * 5 + g) * HEAD:(c * 5 + g + 1) * HEAD]
            if g <= GROUP:
                x = x * cos + pltpu.roll(x, HEAD // 2, 1) * sin
            x = round_bf16(x)
            if g < GROUP:
                q_ref[:, (c * GROUP + g) * HEAD:(c * GROUP + g + 1) * HEAD] = x
            else:
                at = (c * 2 + g - GROUP) * HEAD
                kv_ref[:, at:at + HEAD] = x


def attend(sparse, base, count, start, pos_ref, q8, kbuf, vbuf, s8, acc8, ml8):
    t, s = lax.axis_index("tp"), lax.axis_index("sp")
    row = lax.broadcasted_iota(jnp.int32, (8, KV * SLOTS), 0)
    col = lax.broadcasted_iota(jnp.int32, (8, KV * SLOTS), 1)
    slot = s * SLOTS + col // KV
    same = (col % KV) == row // GROUP
    vertical = (slot // BLOCK_SIZE + (t * HEADS + row) + 1) % VERT_STRIDE == 0
    for j in range(count):
        at = slice((start + j) * 8, (start + j) * 8 + 8)
        b = base + j
        p = pos_ref[b]
        queries = q8[pl.ds(pl.multiple_of(b * 8, 8), 8), :].astype(BF16)
        scores = lax.dot_general(queries, kbuf[b], (((1,), (1,)), ((), ())), preferred_element_type=F32)
        keep = (slot < p) & same
        if sparse:
            near = (p // BLOCK_SIZE - slot // BLOCK_SIZE) < LOCAL_BLOCKS
            keep = keep & (near | vertical)
        s8[at, :] = jnp.where(keep, scores * (1.0 / HEAD), -jnp.inf)
    for r in range(count // 8):
        at = slice(start * 8 + r * SEQS, start * 8 + (r + 1) * SEQS)
        scores = s8[at, :]
        peak = jnp.maximum(jnp.max(scores, axis=-1, keepdims=True), MASKED)
        weights = jnp.exp(scores - peak)
        s8[at, :] = weights
        total = jnp.sum(weights, axis=-1, keepdims=True)
        low = lax.broadcasted_iota(jnp.int32, (SEQS, HEAD), 1) < HEADS
        ml8[at, :] = jnp.where(low, peak, total)
    for j in range(count):
        at = slice((start + j) * 8, (start + j) * 8 + 8)
        acc8[at, :] = dot(s8[at, :].astype(BF16), vbuf[base + j])


def pack_stats(stats, base, count, start, acc8, ml8):
    rows = slice(base, base + count) if isinstance(base, int) else pl.ds(pl.multiple_of(base, count), count)
    lane = lax.broadcasted_iota(jnp.int32, (count, HEAD), 1)
    tail = jnp.zeros((count, HEAD), F32)
    for h in range(HEADS):
        at = pl.ds(start * 8 + h, count, stride=8)
        stats[rows, h * HEAD:(h + 1) * HEAD] = acc8[at, :]
        tail = jnp.where((lane == h) | (lane == HEADS + h), ml8[at, :], tail)
    stats[rows, HEADS * HEAD:] = tail


def put_new_rows(group, pos_ref, kv_ref, kbuf, vbuf):
    s = lax.axis_index("sp")
    row = lax.broadcasted_iota(jnp.int32, (16, HEAD), 0)
    fresh_rows = kv_ref[pl.ds(pl.multiple_of(group * GRP, GRP), GRP), :]
    for j in range(GRP):
        b = group * GRP + j
        local = pos_ref[b] - s * SLOTS
        inside = jnp.where((local >= 0) & (local < SLOTS), 1, 0)
        local = jnp.clip(local, 0, SLOTS - 1)
        at = pl.ds(pl.multiple_of((local // 8) * 16, 16), 16)
        target = jnp.where(inside == 1, local % 8, 99)
        hit = (row // KV) == target
        for i, buf in enumerate((kbuf, vbuf)):
            first, second = (fresh_rows[j:j + 1, (2 * c + i) * HEAD:(2 * c + i + 1) * HEAD] for c in range(KV))
            fresh = jnp.where(row % KV == 0, first, second)
            buf[b, at, :] = jnp.where(hit, fresh, buf[b, at, :].astype(F32)).astype(BF16)


def stream_cache(layer, src_pair, buf_pair, dst_pair, sems):
    def copies(g, out):
        at = pl.ds(g * GRP, GRP)
        if out:
            return [pltpu.make_async_copy(buf.at[at], dst.at[layer, at], sems.at[2 + i, g])
                    for i, (buf, dst) in enumerate(zip(buf_pair, dst_pair))]
        return [pltpu.make_async_copy(src.at[layer, at], buf.at[at], sems.at[i, g])
                for i, (src, buf) in enumerate(zip(src_pair, buf_pair))]

    return copies


def store_cache(copies, pos_ref, kv_ref, kbuf, vbuf):
    def one_group(g, carry):
        for copy in copies(g, 0):
            copy.wait()
        put_new_rows(g, pos_ref, kv_ref, kbuf, vbuf)
        for copy in copies(g, 1):
            copy.start()
        return carry

    lax.fori_loop(0, NGRP, one_group, 0)


def drain_cache(copies):
    def drain(g, carry):
        for copy in copies(g, 1):
            copy.wait()
        return carry

    lax.fori_loop(0, NGRP, drain, 0)


def fetch(sources, targets, sems):
    copies = [pltpu.make_async_copy(src, dst, sems.at[i]) for i, (src, dst) in enumerate(zip(sources, targets))]
    for copy in copies:
        copy.start()
    return copies


def entry_kernel(pos_hbm, hidden_hbm, gain_hbm, shift_hbm, b_hbm, table_hbm, w_hbm, kc_hbm, vc_hbm,
                 ko_hbm, vo_hbm, q0_hbm, kv0_hbm, stats0_hbm, cos_hbm, sin_hbm,
                 pos_ref, hidden, gain, shift, b_qkv, table, q0, kv0, stats0, cos_rows, sin_rows,
                 wbuf, kbuf, vbuf, u_s, acc, q8, s8, acc8, ml8, w_sem, sems, small):
    first = fetch((pos_hbm, hidden_hbm, gain_hbm, shift_hbm, b_hbm, table_hbm),
                  (pos_ref, hidden, gain, shift, b_qkv, table), small)
    copies = stream_cache(0, (kc_hbm, vc_hbm), (kbuf, vbuf), (ko_hbm, vo_hbm), sems)

    def w_copy(n):
        return pltpu.make_async_copy(w_hbm.at[0, pl.ds(n * CH, CH)], wbuf.at[pl.ds(n * CH, CH)], w_sem.at[n])

    for n in range(NCH):
        w_copy(n).start()

    q8[...] = jnp.zeros_like(q8)
    for copy in first:
        copy.wait()

    def pick_row(b, carry):
        p = pos_ref[b]
        cos_rows[pl.ds(b, 1), :] = table[pl.ds(p, 1), :]
        return carry

    lax.fori_loop(0, SEQS, pick_row, 0)
    both = cos_rows[...]
    other = pltpu.roll(both, HEAD // 2, 1)
    low = lax.broadcasted_iota(jnp.int32, (SEQS, HEAD), 1) < HEAD // 2
    cos_rows[...] = jnp.where(low, both, other)
    sin_rows[...] = jnp.where(low, -other, both)
    u_s[...] = norm_rows(hidden[...].astype(F32), param_row(gain, 0, 0), param_row(shift, 0, 0))
    for n in range(NCH):
        w_copy(n).wait()
        if n == 0:
            for g in range(NGRP):
                for copy in copies(g, 0):
                    copy.start()
        piece = dot(u_s[:, n * CH:(n + 1) * CH], wbuf[n * CH:(n + 1) * CH, :])
        acc[...] = piece + param_row(b_qkv, 0) if n == 0 else acc[...] + piece
    turn_columns(acc, q0, kv0, cos_rows[...], sin_rows[...])
    outs = fetch((q0, kv0, cos_rows, sin_rows), (q0_hbm, kv0_hbm, cos_hbm, sin_hbm), small)
    for h in range(HEADS):
        q8[pl.ds(h, SEQS, stride=8), :] = q0[:, h * HEAD:(h + 1) * HEAD]
    store_cache(copies, pos_ref, kv0, kbuf, vbuf)
    attend(True, 0, SEQS, 0, pos_ref, q8, kbuf, vbuf, s8, acc8, ml8)
    pack_stats(stats0, 0, SEQS, 0, acc8, ml8)
    stats_out = pltpu.make_async_copy(stats0, stats0_hbm, small.at[4])
    stats_out.start()
    drain_cache(copies)
    for copy in outs + [stats_out]:
        copy.wait()


def exit_kernel(pos_hbm, kv_hbm, hid_hbm, kc_hbm, vc_hbm, ka_hbm, va_hbm, hid_out, ko_hbm, vo_hbm,
                kbuf, vbuf, kv, hid, pos_ref, sems, small):
    copies = stream_cache(1, (kc_hbm, vc_hbm), (kbuf, vbuf), (ko_hbm, vo_hbm), sems)
    first = [pltpu.make_async_copy(src, dst, small.at[i])
             for i, (src, dst) in enumerate(((pos_hbm, pos_ref), (kv_hbm, kv), (hid_hbm, hid)))]
    hid_back = pltpu.make_async_copy(hid, hid_out, small.at[3])
    for copy in first:
        copy.start()
    for g in range(NGRP):
        for copy in copies(g, 0):
            copy.start()
    for copy in first:
        copy.wait()
    hid_back.start()
    store_cache(copies, pos_ref, kv, kbuf, vbuf)
    drain_cache(copies)
    hid_back.wait()


def main_kernel(pos_hbm, q0_hbm, kv0_hbm, stats0_hbm, cos_hbm, sin_hbm, hidden_hbm,
                gain_hbm, shift_hbm, bqkv_hbm, bdense_hbm, bup_hbm, bdown_hbm,
                wqkv_hbm, wdense_hbm, wup_hbm, wdown_hbm, kc_hbm, vc_hbm,
                hid, kv1_out,
                pos_ref, q0, kv0, stats0, cos_rows, sin_rows, hidden, gain, shift, b_qkv, b_dense, b_up, b_down, small,
                wqkv, wdense, wup, wdown, kbuf, vbuf,
                mix, part, summed, spread, x_own, o16, u16, h_s, m16, acc, q1, kv1, stats1, fin, q8, s8, acc8, ml8,
                w_sem, kv_sem, mix_send, mix_recv, part_send, part_recv, spread_send, spread_recv,
                q_send, q_recv, fin_send, fin_recv, z_send):
    t, s = lax.axis_index("tp"), lax.axis_index("sp")
    far = (2, 1, 3)
    unsent = {}

    def remote(src, dst, send_sem, recv_sem, axis, peer):
        return pltpu.make_async_remote_copy(src_ref=src, dst_ref=dst, send_sem=send_sem, recv_sem=recv_sem,
                                            device_id={axis: peer}, device_id_type=MESH)

    def send(*args, key=None):
        copy = remote(*args)
        copy.start()
        unsent.setdefault(key, []).append(copy)

    def flush(key):
        for copy in unsent.pop(key):
            copy.wait_send()

    def arrived(*args):
        remote(*args).wait_recv()

    barrier = pltpu.get_barrier_semaphore()
    for axis, me in (("tp", t), ("sp", s)):
        for d in range(1, 4):
            pl.semaphore_signal(barrier, inc=1, device_id={axis: lax.rem(me + d, 4)}, device_id_type=MESH)

    my_rows = pl.ds(pl.multiple_of(s * ROWS, ROWS), ROWS)
    first = fetch((stats0_hbm, pos_hbm, q0_hbm.at[my_rows], kv0_hbm.at[my_rows], cos_hbm.at[my_rows],
                   sin_hbm.at[my_rows], hidden_hbm.at[my_rows], gain_hbm, shift_hbm, bqkv_hbm, bdense_hbm, bup_hbm,
                   bdown_hbm),
                  (stats0, pos_ref, q0, kv0, cos_rows, sin_rows, hidden, gain, shift, b_qkv, b_dense, b_up, b_down),
                  small)
    cols = [pl.ds(n * CH, CH) for n in range(NCH)]

    def dense_copy(layer, n):
        return pltpu.make_async_copy(wdense_hbm.at[layer, :, cols[n]], wdense.at[:, cols[n]], w_sem.at[0, n])

    def up_copy(layer, n):
        return pltpu.make_async_copy(wup_hbm.at[layer, cols[n]], wup.at[cols[n]], w_sem.at[1, n])

    def down_copy(layer, n):
        return pltpu.make_async_copy(wdown_hbm.at[layer, :, cols[n]], wdown.at[:, cols[n]], w_sem.at[2, n])

    def qkv_copy(layer, n):
        return pltpu.make_async_copy(wqkv_hbm.at[layer, cols[n]], wqkv.at[cols[n]], w_sem.at[3, n])

    def k_copy(layer):
        return pltpu.make_async_copy(kc_hbm.at[layer], kbuf, kv_sem.at[0])

    def v_copy(layer):
        return pltpu.make_async_copy(vc_hbm.at[layer], vbuf, kv_sem.at[1])

    q8[...] = jnp.zeros_like(q8)
    for copy in first:
        copy.wait()
    for n in range(NCH):
        dense_copy(0, n).start()
    for n in range(NCH):
        up_copy(0, n).start()
    wide = hidden[...].astype(F32)
    for j in range(4):
        fin[0, j] = wide[OWN * j:OWN * (j + 1)]
    x_own[...] = fin[0, t]
    pl.semaphore_wait(barrier, 6)

    twin = s + 1 - 2 * (s % 2)
    across = (s + 2) % 4
    partners = (twin, across, (twin + 2) % 4)

    def exchange(layer, stats, kinds):
        for kind in kinds:
            peer = partners[kind]
            rows = pl.ds(pl.multiple_of(peer * ROWS, ROWS), ROWS)
            send(stats.at[rows], mix.at[layer, kind], mix_send.at[layer, kind], mix_recv.at[layer, kind], "sp", peer)

    def combine(layer, stats, q_rows, kv_rows):
        for kind in range(3):
            dst = mix.at[layer, kind]
            arrived(dst, dst, mix_send.at[layer, kind], mix_recv.at[layer, kind], "sp", partners[kind])
        shards = [stats[my_rows, :]] + [mix[layer, d] for d in range(3)]
        for h in range(HEADS):
            c = h // GROUP
            q = q_rows[:, h * HEAD:(h + 1) * HEAD]
            k = kv_rows[:, 2 * c * HEAD:(2 * c + 1) * HEAD]
            v = kv_rows[:, (2 * c + 1) * HEAD:(2 * c + 2) * HEAD]
            fresh = jnp.sum(q * k, axis=-1, keepdims=True) * (1.0 / HEAD)
            peaks = [x[:, QW + h:QW + h + 1] for x in shards]
            top = fresh
            for peak in peaks:
                top = jnp.maximum(top, peak)
            scale = jnp.exp(fresh - top)
            num, den = v * scale, scale
            for x, peak in zip(shards, peaks):
                scale = jnp.exp(peak - top)
                num = num + x[:, h * HEAD:(h + 1) * HEAD] * scale
                den = den + x[:, QW + HEADS + h:QW + HEADS + h + 1] * scale
            o16[:, h * HEAD:(h + 1) * HEAD] = (num / den).astype(BF16)

    def reduce_rows(phase, lhs, weights, layer, copy_of):
        turn = phase % 2
        if phase >= 2:
            flush(("part", phase - 2))
        for n in range(NCH):
            copy_of(layer, n).wait()
            piece = dot(lhs[...], weights[:, n * CH:(n + 1) * CH])
            for j in range(4):
                part[turn, j, :, n * CH:(n + 1) * CH] = piece[OWN * j:OWN * (j + 1)]
            for d in far:
                peer = lax.rem(t + d, 4)
                send(part.at[turn, peer, :, cols[n]], summed.at[turn, d - 1, :, cols[n]],
                     part_send.at[phase, d - 1, n], part_recv.at[phase, d - 1, n], "tp", peer, key=("part", phase))

    def sum_rows(phase, n):
        turn = phase % 2
        for d in range(1, 4):
            dst = summed.at[turn, d - 1, :, cols[n]]
            arrived(dst, dst, part_send.at[phase, d - 1, n], part_recv.at[phase, d - 1, n], "tp", lax.rem(t + d, 4))
        at = slice(n * CH, (n + 1) * CH)
        return part[turn, t, :, at] + summed[turn, 0, :, at] + summed[turn, 1, :, at] + summed[turn, 2, :, at]

    def add_rows(phase, bias):
        for n in range(NCH):
            at = slice(n * CH, (n + 1) * CH)
            x_own[:, at] = round_bf16(x_own[:, at] + sum_rows(phase, n) + bias[:, at])

    def spread_rows(phase, layer, which):
        rows = norm_rows(x_own[...], param_row(gain, layer, which), param_row(shift, layer, which))
        spread[phase % 2, t] = rows.astype(F32)
        for n in range(NCH):
            block = spread.at[phase % 2, t, :, cols[n]]
            for d in far:
                send(block, block, spread_send.at[phase, d - 1, n], spread_recv.at[phase, d - 1, n], "tp",
                     lax.rem(t + d, 4), key=("spread", phase))

    def take_rows(phase, n):
        for d in range(1, 4):
            dst = spread.at[phase % 2, lax.rem(t - d + 4, 4), :, cols[n]]
            arrived(dst, dst, spread_send.at[phase, d - 1, n], spread_recv.at[phase, d - 1, n], "tp", lax.rem(t + d, 4))
        at = slice(n * CH, (n + 1) * CH)
        u16[...] = jnp.concatenate([spread[phase % 2, j, :, at] for j in range(4)], axis=0).astype(BF16)

    lane = lax.broadcasted_iota(jnp.int32, (ROWS, 1024), 1)
    pick = (lax.broadcasted_iota(jnp.int32, (256, 128), 0) == 2 * lax.broadcasted_iota(jnp.int32, (256, 128), 1))
    pick = jnp.where(pick, 1.0, 0.0).astype(BF16)

    def finish_layer(layer):
        last = layer == 1
        reduce_rows(2 * layer, o16, wdense, layer, dense_copy)

        if last:
            flush(("spread", 0))

        add_rows(2 * layer, param_row(b_dense, layer))
        spread_rows(2 * layer, layer, 1)
        bias = param_row(b_up, layer)
        for n in range(NCH):
            up_copy(layer, n).wait()
            take_rows(2 * layer, n)
            for c in range(4):
                at = slice(c * 1024, (c + 1) * 1024)
                piece = dot(u16[...], wup[n * CH:(n + 1) * CH, at])
                h_s[:, at] = piece + bias[:, at] if n == 0 else h_s[:, at] + piece
        if not last:
            for n in range(NCH):
                qkv_copy(1, n).start()
        for c in range(4):
            pair = h_s[:, c * 1024:(c + 1) * 1024]
            gate = jnp.minimum(pair, GELU_LIMIT)
            line = jnp.clip(pltpu.roll(pair, 1023, 1), -GELU_LIMIT, GELU_LIMIT)
            act = gate * jax.nn.sigmoid(1.702 * gate) * (line + 1.0)
            act = jnp.where(lane % 2 == 0, act, 0.0).astype(BF16)
            for k in range(4):
                at = slice(c * 512 + k * 128, c * 512 + (k + 1) * 128)
                m16[:, at] = dot(act[:, k * 256:(k + 1) * 256], pick).astype(BF16)
        reduce_rows(2 * layer + 1, m16, wdown, layer, down_copy)
        if not last:
            k_copy(1).start()
            v_copy(1).start()

    exchange(0, stats0, (2, 1, 0))
    for n in range(NCH):
        down_copy(0, n).start()
    combine(0, stats0, q0[...], kv0[...])
    finish_layer(0)

    add_rows(1, param_row(b_down, 0))
    spread_rows(1, 1, 0)
    for n in range(NCH):
        qkv_copy(1, n).wait()
        take_rows(1, n)
        piece = dot(u16[...], wqkv[n * CH:(n + 1) * CH, :])
        acc[...] = piece + param_row(b_qkv, 1) if n == 0 else acc[...] + piece
    for n in range(NCH):
        dense_copy(1, n).start()
    for n in range(NCH):
        up_copy(1, n).start()
    turn_columns(acc, q1.at[s], kv1.at[s], cos_rows[...], sin_rows[...])
    for i, ref in enumerate((q1, kv1)):
        for d in far:
            send(ref.at[s], ref.at[s], q_send.at[i, d - 1], q_recv.at[i, d - 1], "sp", lax.rem(s + d, 4))

    def gathered(i, ref):
        for d in range(1, 4):
            dst = ref.at[lax.rem(s - d + 4, 4)]
            arrived(dst, dst, q_send.at[i, d - 1], q_recv.at[i, d - 1], "sp", lax.rem(s + d, 4))

    gathered(0, q1)
    for i in range(4):
        for h in range(HEADS):
            q8[pl.ds(i * ROWS * 8 + h, ROWS, stride=8), :] = q1[i, :, h * HEAD:(h + 1) * HEAD]
    k_copy(1).wait()
    v_copy(1).wait()
    half = SEQS // 2
    for i, (base, kinds) in enumerate((((1 - s // 2) * half, (2, 1)), ((s // 2) * half, (0,)))):
        attend(False, base, half, i * half, pos_ref, q8, kbuf, vbuf, s8, acc8, ml8)
        pack_stats(stats1, base, half, i * half, acc8, ml8)
        exchange(1, stats1, kinds)
    for n in range(NCH):
        down_copy(1, n).start()
    combine(1, stats1, q1[s], kv1[s])
    finish_layer(1)

    diagonal = lax.rem(twin + 2, 4)

    def hop(kind, block, i, n, axis, peer):
        return block, block, fin_send.at[kind, i, n], fin_recv.at[kind, i, n], axis, peer

    bias = param_row(b_down, 1)
    for n in range(NCH):
        at = slice(n * CH, (n + 1) * CH)
        fin[s, t, :, at] = round_bf16(x_own[:, at] + sum_rows(3, n) + bias[:, at])
        block = fin.at[s, t, :, cols[n]]
        for d in far:
            send(block, block, z_send.at[d - 1, n], fin_recv.at[0, d, n], "tp", lax.rem(t + d, 4))
        send(*hop(1, block, 0, n, "sp", across))
        send(*hop(2, block, 0, n, "sp", twin))
    for n in range(NCH):
        for d in (1, 3, 2):
            block = fin.at[s, lax.rem(t - d + 4, 4), :, cols[n]]
            arrived(*hop(0, block, d, n, "tp", lax.rem(t + d, 4)))
            send(*hop(1, block, d, n, "sp", across))
            send(*hop(2, block, d, n, "sp", twin))
    for n in range(NCH):
        for d in range(4):
            block = fin.at[across, lax.rem(t - d + 4, 4), :, cols[n]]
            arrived(*hop(1, block, d, n, "sp", across))
            send(*hop(3, block, d, n, "sp", twin))
    gathered(1, kv1)
    for i in range(4):
        kv1_out[i * ROWS:(i + 1) * ROWS, :] = kv1[i]
    for n in range(NCH):
        for d in range(4):
            arrived(*hop(2, fin.at[twin, lax.rem(t - d + 4, 4), :, cols[n]], d, n, "sp", twin))
            arrived(*hop(3, fin.at[diagonal, lax.rem(t - d + 4, 4), :, cols[n]], d, n, "sp", twin))
    for i in range(4):
        hid[i * ROWS:(i + 1) * ROWS, :] = jnp.concatenate([fin[i, j] for j in range(4)], axis=0).astype(BF16)
    for key in list(unsent):
        flush(key)


def solution(mesh):
    cache_spec = P(None, "dp", "sp", "tp", None)
    in_specs = (P("dp", None), P("dp"), cache_spec, cache_spec, P(), P(), P(None, None, "tp"), P(None, "tp"),
                P(None, "tp", None), P(), P(None, None, "tp"), P(None, "tp"), P(None, "tp", None), P())
    out_specs = (P("dp", None), cache_spec, cache_spec)
    table = rope_table()
    vmem, hbm = (pl.BlockSpec(memory_space=m) for m in (pltpu.VMEM, pl.ANY))
    dma = pltpu.SemaphoreType.DMA

    def device_step(hidden, positions, k_cache, v_cache, ln_gain, ln_bias, w_qkv, b_qkv, w_dense, b_dense,
                    w_up, b_up, w_down, b_down):
        flat = (2, SEQS, SLOTS * KV, HEAD)
        kc, vc = k_cache.reshape(flat), v_cache.reshape(flat)
        cache = jax.ShapeDtypeStruct(flat, BF16)
        row8 = [pltpu.VMEM((SEQS * 8, n * HEAD), F32) for n in (1, 2, 1, 1)]
        buffers = [pltpu.VMEM(flat[1:], BF16)] * 2
        rows = [jax.ShapeDtypeStruct((SEQS, n), F32) for n in (QW, KVW, STAT, HEAD, HEAD)]
        big = pltpu.CompilerParams(vmem_limit_bytes=VMEM_MAX)
        ko, vo, q0, kv0, stats0, cos_rows, sin_rows = pl.pallas_call(
            entry_kernel,
            out_shape=(cache, cache, *rows),
            in_specs=[hbm] * 9,
            out_specs=(hbm,) * 7,
            scratch_shapes=[pltpu.SMEM((SEQS,), jnp.int32), pltpu.VMEM((SEQS, D), BF16), pltpu.VMEM((2, 2, D), BF16),
                            pltpu.VMEM((2, 2, D), BF16), pltpu.VMEM((2, QKV), BF16), pltpu.VMEM((SEQ_LEN, HEAD), F32)]
            + [pltpu.VMEM(x.shape, F32) for x in rows] + [pltpu.VMEM((D, QKV), BF16)] + buffers
            + [pltpu.VMEM((SEQS, D), BF16), pltpu.VMEM((SEQS, QKV), F32)] + row8 + [dma((NCH,)), dma((4, NGRP)), dma((6,))],
            compiler_params=big,
            name="entry",
        )(positions, hidden, ln_gain, ln_bias, b_qkv, table, w_qkv, kc, vc)

        hid, kv1 = pl.pallas_call(
            main_kernel,
            out_shape=(jax.ShapeDtypeStruct((SEQS, D), BF16), rows[1]),
            in_specs=[hbm] * 19,
            out_specs=(vmem, vmem),
            scratch_shapes=[
                pltpu.SMEM((SEQS,), jnp.int32), pltpu.VMEM((ROWS, QW), F32), pltpu.VMEM((ROWS, KVW), F32),
                pltpu.VMEM((SEQS, STAT), F32), pltpu.VMEM((ROWS, HEAD), F32), pltpu.VMEM((ROWS, HEAD), F32),
                pltpu.VMEM((ROWS, D), BF16), pltpu.VMEM((2, 2, D), BF16), pltpu.VMEM((2, 2, D), BF16),
                pltpu.VMEM((2, QKV), BF16), pltpu.VMEM((2, D), BF16), pltpu.VMEM((2, UP), BF16),
                pltpu.VMEM((2, D), BF16), dma((13,)),
                pltpu.VMEM((D, QKV), BF16), pltpu.VMEM((QW, D), BF16), pltpu.VMEM((D, UP), BF16),
                pltpu.VMEM((FF, D), BF16)] + buffers + [
                pltpu.VMEM((2, 3, ROWS, STAT), F32),
                pltpu.VMEM((2, 4, OWN, D), F32),
                pltpu.VMEM((2, 3, OWN, D), F32),
                pltpu.VMEM((2, 4, OWN, D), F32),
                pltpu.VMEM((OWN, D), F32),
                pltpu.VMEM((ROWS, QW), BF16),
                pltpu.VMEM((ROWS, CH), BF16),
                pltpu.VMEM((ROWS, UP), F32),
                pltpu.VMEM((ROWS, FF), BF16),
                pltpu.VMEM((ROWS, QKV), F32),
                pltpu.VMEM((4, ROWS, QW), F32),
                pltpu.VMEM((4, ROWS, KVW), F32),
                pltpu.VMEM((SEQS, STAT), F32),
                pltpu.VMEM((4, 4, OWN, D), F32),
            ] + row8 + [
                dma((4, NCH)), dma((2,)), dma((2, 3)), dma((2, 3)), dma((4, 3, NCH)), dma((4, 3, NCH)),
                dma((3, 3, NCH)), dma((3, 3, NCH)), dma((2, 3)), dma((2, 3)), dma((4, 4, NCH)), dma((4, 4, NCH)),
                dma((3, NCH))],
            compiler_params=pltpu.CompilerParams(vmem_limit_bytes=VMEM_MAX, collective_id=0, has_side_effects=True),
            name="main",
        )(positions, q0, kv0, stats0, cos_rows, sin_rows, hidden, ln_gain, ln_bias, b_qkv, b_dense, b_up, b_down,
          w_qkv, w_dense, w_up, w_down, kc, vc)

        hidden_out, ko, vo = pl.pallas_call(
            exit_kernel,
            out_shape=(jax.ShapeDtypeStruct((SEQS, D), BF16), cache, cache),
            in_specs=[hbm] * 7,
            out_specs=(hbm, hbm, hbm),
            scratch_shapes=buffers + [pltpu.VMEM((SEQS, KVW), F32), pltpu.VMEM((SEQS, D), BF16),
                                      pltpu.SMEM((SEQS,), jnp.int32), dma((4, NGRP)), dma((4,))],
            input_output_aliases={5: 1, 6: 2},
            compiler_params=big,
            name="exit",
        )(positions, kv1, hid, kc, vc, ko, vo)
        return hidden_out, ko.reshape(k_cache.shape), vo.reshape(v_cache.shape)

    return jax.shard_map(device_step, mesh=mesh, in_specs=in_specs, out_specs=out_specs, check_vma=False)
```

```python
import functools

import jax
import jax.numpy as jnp
import numpy as np
from jax import lax
from jax.experimental import pallas as pl
from jax.experimental.pallas import tpu as pltpu
from jax.sharding import PartitionSpec as P

MESH = pl.DeviceIdType.MESH
F32 = jnp.float32
BF16 = jnp.bfloat16
BLOCK_SIZE = 64
LOCAL_BLOCKS = 16
VERT_STRIDE = 8
ROPE_THETA = 1000000.0
GELU_LIMIT = 20.0
NORM_EPS = 0.00001
MASKED = -1e30

SEQS = 64
ROWS = 16
OWN = 4
SEQ_LEN = 512
SLOTS = 128
D = 3072
HEAD = 128
KV = 2
GROUP = 3
HEADS = KV * GROUP
QKV = 1280
QW = HEADS * HEAD
KVW = 2 * KV * HEAD
UP = 4096
FF = 2048
STAT = HEADS * HEAD + HEAD
NCH = 4
CH = D // NCH
GRP = 8
NGRP = SEQS // GRP
VMEM_MAX = 67043328


def rope_table():
    half = HEAD // 2
    inv = (ROPE_THETA ** (-np.arange(half).astype(np.float32) * np.float32(2.0 / HEAD))).astype(np.float32)
    angle = (np.arange(SEQ_LEN).astype(np.float32)[:, None] * inv[None, :]).astype(np.float64)
    cos, sin = np.cos(angle).astype(np.float32), np.sin(angle).astype(np.float32)
    return np.concatenate([cos, sin], 1)


def norm_rows(wide, gain, shift):
    mean = jnp.mean(wide, axis=-1, keepdims=True)
    centred = wide - mean
    var = jnp.mean(centred * centred, axis=-1, keepdims=True)
    return (centred * lax.rsqrt(var + NORM_EPS) * gain + shift).astype(BF16)


def param_row(ref, layer, which=None):
    rows = ref[...] if which is None else ref[layer]
    pick = layer if which is None else which
    return rows.astype(F32)[pick:pick + 1]


def round_bf16(x):
    return x.astype(BF16).astype(F32)


def dot(a, b):
    return jnp.dot(a, b, preferred_element_type=F32)


def turn_columns(acc, q_ref, kv_ref, cos, sin):
    for c in range(KV):
        for g in range(GROUP + 2):
            x = acc[:, (c * 5 + g) * HEAD:(c * 5 + g + 1) * HEAD]
            if g <= GROUP:
                x = x * cos + pltpu.roll(x, HEAD // 2, 1) * sin
            x = round_bf16(x)
            if g < GROUP:
                q_ref[:, (c * GROUP + g) * HEAD:(c * GROUP + g + 1) * HEAD] = x
            else:
                at = (c * 2 + g - GROUP) * HEAD
                kv_ref[:, at:at + HEAD] = x


def attend(sparse, base, count, start, pos_ref, q8, kbuf, vbuf, s8, acc8, ml8):
    t, s = lax.axis_index("tp"), lax.axis_index("sp")
    row = lax.broadcasted_iota(jnp.int32, (8, KV * SLOTS), 0)
    col = lax.broadcasted_iota(jnp.int32, (8, KV * SLOTS), 1)
    slot = s * SLOTS + col // KV
    same = (col % KV) == row // GROUP
    vertical = (slot // BLOCK_SIZE + (t * HEADS + row) + 1) % VERT_STRIDE == 0
    for j in range(count):
        at = slice((start + j) * 8, (start + j) * 8 + 8)
        b = base + j
        p = pos_ref[b]
        queries = q8[pl.ds(pl.multiple_of(b * 8, 8), 8), :].astype(BF16)
        scores = lax.dot_general(queries, kbuf[b], (((1,), (1,)), ((), ())), preferred_element_type=F32)
        keep = (slot < p) & same
        if sparse:
            near = (p // BLOCK_SIZE - slot // BLOCK_SIZE) < LOCAL_BLOCKS
            keep = keep & (near | vertical)
        s8[at, :] = jnp.where(keep, scores * (1.0 / HEAD), -jnp.inf)
    for r in range(count // 8):
        at = slice(start * 8 + r * SEQS, start * 8 + (r + 1) * SEQS)
        scores = s8[at, :]
        peak = jnp.maximum(jnp.max(scores, axis=-1, keepdims=True), MASKED)
        weights = jnp.exp(scores - peak)
        s8[at, :] = weights
        total = jnp.sum(weights, axis=-1, keepdims=True)
        low = lax.broadcasted_iota(jnp.int32, (SEQS, HEAD), 1) < HEADS
        ml8[at, :] = jnp.where(low, peak, total)
    for j in range(count):
        at = slice((start + j) * 8, (start + j) * 8 + 8)
        acc8[at, :] = dot(s8[at, :].astype(BF16), vbuf[base + j])


def pack_stats(stats, base, count, start, acc8, ml8):
    rows = slice(base, base + count) if isinstance(base, int) else pl.ds(pl.multiple_of(base, count), count)
    lane = lax.broadcasted_iota(jnp.int32, (count, HEAD), 1)
    tail = jnp.zeros((count, HEAD), F32)
    for h in range(HEADS):
        at = pl.ds(start * 8 + h, count, stride=8)
        stats[rows, h * HEAD:(h + 1) * HEAD] = acc8[at, :]
        tail = jnp.where((lane == h) | (lane == HEADS + h), ml8[at, :], tail)
    stats[rows, HEADS * HEAD:] = tail


def put_new_rows(group, pos_ref, kv_ref, kbuf, vbuf):
    s = lax.axis_index("sp")
    row = lax.broadcasted_iota(jnp.int32, (16, HEAD), 0)
    fresh_rows = kv_ref[pl.ds(pl.multiple_of(group * GRP, GRP), GRP), :]
    for j in range(GRP):
        b = group * GRP + j
        local = pos_ref[b] - s * SLOTS
        inside = jnp.where((local >= 0) & (local < SLOTS), 1, 0)
        local = jnp.clip(local, 0, SLOTS - 1)
        at = pl.ds(pl.multiple_of((local // 8) * 16, 16), 16)
        target = jnp.where(inside == 1, local % 8, 99)
        hit = (row // KV) == target
        for i, buf in enumerate((kbuf, vbuf)):
            first, second = (fresh_rows[j:j + 1, (2 * c + i) * HEAD:(2 * c + i + 1) * HEAD] for c in range(KV))
            fresh = jnp.where(row % KV == 0, first, second)
            buf[b, at, :] = jnp.where(hit, fresh, buf[b, at, :].astype(F32)).astype(BF16)


def stream_cache(layer, src_pair, buf_pair, dst_pair, sems):
    def copies(g, out):
        at = pl.ds(g * GRP, GRP)
        if out:
            return [pltpu.make_async_copy(buf.at[at], dst.at[layer, at], sems.at[2 + i, g])
                    for i, (buf, dst) in enumerate(zip(buf_pair, dst_pair))]
        return [pltpu.make_async_copy(src.at[layer, at], buf.at[at], sems.at[i, g])
                for i, (src, buf) in enumerate(zip(src_pair, buf_pair))]

    return copies


def store_cache(copies, pos_ref, kv_ref, kbuf, vbuf):
    def one_group(g, carry):
        for copy in copies(g, 0):
            copy.wait()
        put_new_rows(g, pos_ref, kv_ref, kbuf, vbuf)
        for copy in copies(g, 1):
            copy.start()
        return carry

    lax.fori_loop(0, NGRP, one_group, 0)


def drain_cache(copies):
    def drain(g, carry):
        for copy in copies(g, 1):
            copy.wait()
        return carry

    lax.fori_loop(0, NGRP, drain, 0)


def fetch(sources, targets, sems):
    copies = [pltpu.make_async_copy(src, dst, sems.at[i]) for i, (src, dst) in enumerate(zip(sources, targets))]
    for copy in copies:
        copy.start()
    return copies


def entry_kernel(pos_hbm, hidden_hbm, gain_hbm, shift_hbm, b_hbm, table_hbm, w_hbm, kc_hbm, vc_hbm,
                 ko_hbm, vo_hbm, q0_hbm, kv0_hbm, stats0_hbm, cos_hbm, sin_hbm,
                 pos_ref, hidden, gain, shift, b_qkv, table, q0, kv0, stats0, cos_rows, sin_rows,
                 wbuf, kbuf, vbuf, u_s, acc, q8, s8, acc8, ml8, w_sem, sems, small):
    first = fetch((pos_hbm, hidden_hbm, gain_hbm, shift_hbm, b_hbm, table_hbm),
                  (pos_ref, hidden, gain, shift, b_qkv, table), small)
    copies = stream_cache(0, (kc_hbm, vc_hbm), (kbuf, vbuf), (ko_hbm, vo_hbm), sems)

    def w_copy(n):
        return pltpu.make_async_copy(w_hbm.at[0, pl.ds(n * CH, CH)], wbuf.at[pl.ds(n * CH, CH)], w_sem.at[n])

    for n in range(NCH):
        w_copy(n).start()

    q8[...] = jnp.zeros_like(q8)
    for copy in first:
        copy.wait()

    def pick_row(b, carry):
        p = pos_ref[b]
        cos_rows[pl.ds(b, 1), :] = table[pl.ds(p, 1), :]
        return carry

    lax.fori_loop(0, SEQS, pick_row, 0)
    both = cos_rows[...]
    other = pltpu.roll(both, HEAD // 2, 1)
    low = lax.broadcasted_iota(jnp.int32, (SEQS, HEAD), 1) < HEAD // 2
    cos_rows[...] = jnp.where(low, both, other)
    sin_rows[...] = jnp.where(low, -other, both)
    u_s[...] = norm_rows(hidden[...].astype(F32), param_row(gain, 0, 0), param_row(shift, 0, 0))
    for n in range(NCH):
        w_copy(n).wait()
        if n == 0:
            for g in range(NGRP):
                for copy in copies(g, 0):
                    copy.start()
        piece = dot(u_s[:, n * CH:(n + 1) * CH], wbuf[n * CH:(n + 1) * CH, :])
        acc[...] = piece + param_row(b_qkv, 0) if n == 0 else acc[...] + piece
    turn_columns(acc, q0, kv0, cos_rows[...], sin_rows[...])
    outs = fetch((q0, kv0, cos_rows, sin_rows), (q0_hbm, kv0_hbm, cos_hbm, sin_hbm), small)
    for h in range(HEADS):
        q8[pl.ds(h, SEQS, stride=8), :] = q0[:, h * HEAD:(h + 1) * HEAD]
    store_cache(copies, pos_ref, kv0, kbuf, vbuf)
    attend(True, 0, SEQS, 0, pos_ref, q8, kbuf, vbuf, s8, acc8, ml8)
    pack_stats(stats0, 0, SEQS, 0, acc8, ml8)
    stats_out = pltpu.make_async_copy(stats0, stats0_hbm, small.at[4])
    stats_out.start()
    drain_cache(copies)
    for copy in outs + [stats_out]:
        copy.wait()


def exit_kernel(pos_hbm, kv_hbm, hid_hbm, kc_hbm, vc_hbm, ka_hbm, va_hbm, hid_out, ko_hbm, vo_hbm,
                kbuf, vbuf, kv, hid, pos_ref, sems, small):
    copies = stream_cache(1, (kc_hbm, vc_hbm), (kbuf, vbuf), (ko_hbm, vo_hbm), sems)
    first = [pltpu.make_async_copy(src, dst, small.at[i])
             for i, (src, dst) in enumerate(((pos_hbm, pos_ref), (kv_hbm, kv), (hid_hbm, hid)))]
    hid_back = pltpu.make_async_copy(hid, hid_out, small.at[3])
    for copy in first:
        copy.start()
    for g in range(NGRP):
        for copy in copies(g, 0):
            copy.start()
    for copy in first:
        copy.wait()
    hid_back.start()
    store_cache(copies, pos_ref, kv, kbuf, vbuf)
    drain_cache(copies)
    hid_back.wait()


def main_kernel(pos_hbm, q0_hbm, kv0_hbm, stats0_hbm, cos_hbm, sin_hbm, hidden_hbm,
                gain_hbm, shift_hbm, bqkv_hbm, bdense_hbm, bup_hbm, bdown_hbm,
                wqkv_hbm, wdense_hbm, wup_hbm, wdown_hbm, kc_hbm, vc_hbm,
                hid, kv1_out,
                pos_ref, q0, kv0, stats0, cos_rows, sin_rows, hidden, gain, shift, b_qkv, b_dense, b_up, b_down, small,
                wqkv, wdense, wup, wdown, kbuf, vbuf,
                mix, part, summed, spread, x_own, o16, u16, h_s, m16, acc, q1, kv1, stats1, fin, q8, s8, acc8, ml8,
                w_sem, kv_sem, mix_send, mix_recv, part_send, part_recv, spread_send, spread_recv,
                q_send, q_recv, fin_send, fin_recv, z_send):
    t, s = lax.axis_index("tp"), lax.axis_index("sp")
    far = (2, 1, 3)
    unsent = {}

    def remote(src, dst, send_sem, recv_sem, axis, peer):
        return pltpu.make_async_remote_copy(src_ref=src, dst_ref=dst, send_sem=send_sem, recv_sem=recv_sem,
                                            device_id={axis: peer}, device_id_type=MESH)

    def send(*args, key=None):
        copy = remote(*args)
        copy.start()
        unsent.setdefault(key, []).append(copy)

    def flush(key):
        for copy in unsent.pop(key):
            copy.wait_send()

    def arrived(*args):
        remote(*args).wait_recv()

    barrier = pltpu.get_barrier_semaphore()
    for axis, me in (("tp", t), ("sp", s)):
        for d in range(1, 4):
            pl.semaphore_signal(barrier, inc=1, device_id={axis: lax.rem(me + d, 4)}, device_id_type=MESH)

    my_rows = pl.ds(pl.multiple_of(s * ROWS, ROWS), ROWS)
    first = fetch((stats0_hbm, pos_hbm, q0_hbm.at[my_rows], kv0_hbm.at[my_rows], cos_hbm.at[my_rows],
                   sin_hbm.at[my_rows], hidden_hbm.at[my_rows], gain_hbm, shift_hbm, bqkv_hbm, bdense_hbm, bup_hbm,
                   bdown_hbm),
                  (stats0, pos_ref, q0, kv0, cos_rows, sin_rows, hidden, gain, shift, b_qkv, b_dense, b_up, b_down),
                  small)
    cols = [pl.ds(n * CH, CH) for n in range(NCH)]

    def dense_copy(layer, n):
        return pltpu.make_async_copy(wdense_hbm.at[layer, :, cols[n]], wdense.at[:, cols[n]], w_sem.at[0, n])

    def up_copy(layer, n):
        return pltpu.make_async_copy(wup_hbm.at[layer, cols[n]], wup.at[cols[n]], w_sem.at[1, n])

    def down_copy(layer, n):
        return pltpu.make_async_copy(wdown_hbm.at[layer, :, cols[n]], wdown.at[:, cols[n]], w_sem.at[2, n])

    def qkv_copy(layer, n):
        return pltpu.make_async_copy(wqkv_hbm.at[layer, cols[n]], wqkv.at[cols[n]], w_sem.at[3, n])

    def k_copy(layer):
        return pltpu.make_async_copy(kc_hbm.at[layer], kbuf, kv_sem.at[0])

    def v_copy(layer):
        return pltpu.make_async_copy(vc_hbm.at[layer], vbuf, kv_sem.at[1])

    q8[...] = jnp.zeros_like(q8)
    for copy in first:
        copy.wait()
    for n in range(NCH):
        dense_copy(0, n).start()
    for n in range(NCH):
        up_copy(0, n).start()
    wide = hidden[...].astype(F32)
    for j in range(4):
        fin[0, j] = wide[OWN * j:OWN * (j + 1)]
    x_own[...] = fin[0, t]
    pl.semaphore_wait(barrier, 6)

    twin = s + 1 - 2 * (s % 2)
    across = (s + 2) % 4
    partners = (twin, across, (twin + 2) % 4)

    def exchange(layer, stats, kinds):
        for kind in kinds:
            peer = partners[kind]
            rows = pl.ds(pl.multiple_of(peer * ROWS, ROWS), ROWS)
            send(stats.at[rows], mix.at[layer, kind], mix_send.at[layer, kind], mix_recv.at[layer, kind], "sp", peer)

    def combine(layer, stats, q_rows, kv_rows):
        news = []
        for h in range(HEADS):
            k = kv_rows[:, 2 * (h // GROUP) * HEAD:(2 * (h // GROUP) + 1) * HEAD]
            news.append(jnp.sum(q_rows[:, h * HEAD:(h + 1) * HEAD] * k, axis=-1, keepdims=True) * (1.0 / HEAD))
        for kind in range(3):
            dst = mix.at[layer, kind]
            arrived(dst, dst, mix_send.at[layer, kind], mix_recv.at[layer, kind], "sp", partners[kind])
        shards = [stats[my_rows, :]] + [mix[layer, d] for d in range(3)]
        for h in range(HEADS):
            c = h // GROUP
            v = kv_rows[:, (2 * c + 1) * HEAD:(2 * c + 2) * HEAD]
            fresh = news[h]
            peaks = [x[:, QW + h:QW + h + 1] for x in shards]
            top = fresh
            for peak in peaks:
                top = jnp.maximum(top, peak)
            scale = jnp.exp(fresh - top)
            num, den = v * scale, scale
            for x, peak in zip(shards, peaks):
                scale = jnp.exp(peak - top)
                num = num + x[:, h * HEAD:(h + 1) * HEAD] * scale
                den = den + x[:, QW + HEADS + h:QW + HEADS + h + 1] * scale
            o16[:, h * HEAD:(h + 1) * HEAD] = (num / den).astype(BF16)

    def reduce_rows(phase, lhs, weights, layer, copy_of):
        turn = phase % 2
        if phase >= 2:
            flush(("part", phase - 2))
        for n in range(NCH):
            copy_of(layer, n).wait()
            piece = dot(lhs[...], weights[:, n * CH:(n + 1) * CH])
            for j in range(4):
                part[turn, j, :, n * CH:(n + 1) * CH] = piece[OWN * j:OWN * (j + 1)]
            for d in far:
                peer = lax.rem(t + d, 4)
                send(part.at[turn, peer, :, cols[n]], summed.at[turn, d - 1, :, cols[n]],
                     part_send.at[phase, d - 1, n], part_recv.at[phase, d - 1, n], "tp", peer, key=("part", phase))

    def sum_rows(phase, n):
        turn = phase % 2
        for d in range(1, 4):
            dst = summed.at[turn, d - 1, :, cols[n]]
            arrived(dst, dst, part_send.at[phase, d - 1, n], part_recv.at[phase, d - 1, n], "tp", lax.rem(t + d, 4))
        at = slice(n * CH, (n + 1) * CH)
        return part[turn, t, :, at] + summed[turn, 0, :, at] + summed[turn, 1, :, at] + summed[turn, 2, :, at]

    def add_rows(phase, bias):
        for n in range(NCH):
            at = slice(n * CH, (n + 1) * CH)
            x_own[:, at] = round_bf16(x_own[:, at] + sum_rows(phase, n) + bias[:, at])

    def spread_rows(phase, layer, which):
        rows = norm_rows(x_own[...], param_row(gain, layer, which), param_row(shift, layer, which))
        spread[phase % 2, t] = rows.astype(F32)
        for n in range(NCH):
            block = spread.at[phase % 2, t, :, cols[n]]
            for d in far:
                send(block, block, spread_send.at[phase, d - 1, n], spread_recv.at[phase, d - 1, n], "tp",
                     lax.rem(t + d, 4), key=("spread", phase))

    def take_rows(phase, n):
        for d in range(1, 4):
            dst = spread.at[phase % 2, lax.rem(t - d + 4, 4), :, cols[n]]
            arrived(dst, dst, spread_send.at[phase, d - 1, n], spread_recv.at[phase, d - 1, n], "tp", lax.rem(t + d, 4))
        at = slice(n * CH, (n + 1) * CH)
        u16[...] = jnp.concatenate([spread[phase % 2, j, :, at] for j in range(4)], axis=0).astype(BF16)

    lane = lax.broadcasted_iota(jnp.int32, (ROWS, 1024), 1)
    pick = (lax.broadcasted_iota(jnp.int32, (256, 128), 0) == 2 * lax.broadcasted_iota(jnp.int32, (256, 128), 1))
    pick = jnp.where(pick, 1.0, 0.0).astype(BF16)

    def finish_layer(layer):
        last = layer == 1
        reduce_rows(2 * layer, o16, wdense, layer, dense_copy)

        if last:
            flush(("spread", 0))

        add_rows(2 * layer, param_row(b_dense, layer))
        spread_rows(2 * layer, layer, 1)
        bias = param_row(b_up, layer)
        for n in range(NCH):
            up_copy(layer, n).wait()
            take_rows(2 * layer, n)
            for c in range(4):
                at = slice(c * 1024, (c + 1) * 1024)
                piece = dot(u16[...], wup[n * CH:(n + 1) * CH, at])
                h_s[:, at] = piece + bias[:, at] if n == 0 else h_s[:, at] + piece
        if not last:
            for n in range(NCH):
                qkv_copy(1, n).start()
        for c in range(4):
            pair = h_s[:, c * 1024:(c + 1) * 1024]
            gate = jnp.minimum(pair, GELU_LIMIT)
            line = jnp.clip(pltpu.roll(pair, 1023, 1), -GELU_LIMIT, GELU_LIMIT)
            act = gate * jax.nn.sigmoid(1.702 * gate) * (line + 1.0)
            act = jnp.where(lane % 2 == 0, act, 0.0).astype(BF16)
            for k in range(4):
                at = slice(c * 512 + k * 128, c * 512 + (k + 1) * 128)
                m16[:, at] = dot(act[:, k * 256:(k + 1) * 256], pick).astype(BF16)
        reduce_rows(2 * layer + 1, m16, wdown, layer, down_copy)
        if not last:
            k_copy(1).start()
            v_copy(1).start()

    exchange(0, stats0, (2, 1, 0))
    for n in range(NCH):
        down_copy(0, n).start()
    combine(0, stats0, q0[...], kv0[...])
    finish_layer(0)

    add_rows(1, param_row(b_down, 0))
    spread_rows(1, 1, 0)
    for n in range(NCH):
        qkv_copy(1, n).wait()
        take_rows(1, n)
        piece = dot(u16[...], wqkv[n * CH:(n + 1) * CH, :])
        acc[...] = piece + param_row(b_qkv, 1) if n == 0 else acc[...] + piece
    for n in range(NCH):
        dense_copy(1, n).start()
    for n in range(NCH):
        up_copy(1, n).start()
    turn_columns(acc, q1.at[s], kv1.at[s], cos_rows[...], sin_rows[...])
    for i, ref in enumerate((q1, kv1)):
        for d in far:
            send(ref.at[s], ref.at[s], q_send.at[i, d - 1], q_recv.at[i, d - 1], "sp", lax.rem(s + d, 4))

    def gathered(i, ref):
        for d in range(1, 4):
            dst = ref.at[lax.rem(s - d + 4, 4)]
            arrived(dst, dst, q_send.at[i, d - 1], q_recv.at[i, d - 1], "sp", lax.rem(s + d, 4))

    gathered(0, q1)
    for i in range(4):
        for h in range(HEADS):
            q8[pl.ds(i * ROWS * 8 + h, ROWS, stride=8), :] = q1[i, :, h * HEAD:(h + 1) * HEAD]
    k_copy(1).wait()
    v_copy(1).wait()
    half = SEQS // 2
    for i, (base, kinds) in enumerate((((1 - s // 2) * half, (2, 1)), ((s // 2) * half, (0,)))):
        attend(False, base, half, i * half, pos_ref, q8, kbuf, vbuf, s8, acc8, ml8)
        pack_stats(stats1, base, half, i * half, acc8, ml8)
        exchange(1, stats1, kinds)
    for n in range(NCH):
        down_copy(1, n).start()
    combine(1, stats1, q1[s], kv1[s])
    finish_layer(1)

    diagonal = lax.rem(twin + 2, 4)

    def hop(kind, block, i, n, axis, peer):
        return block, block, fin_send.at[kind, i, n], fin_recv.at[kind, i, n], axis, peer

    bias = param_row(b_down, 1)
    for n in range(NCH):
        at = slice(n * CH, (n + 1) * CH)
        fin[s, t, :, at] = round_bf16(x_own[:, at] + sum_rows(3, n) + bias[:, at])
        block = fin.at[s, t, :, cols[n]]
        for d in far:
            send(block, block, z_send.at[d - 1, n], fin_recv.at[0, d, n], "tp", lax.rem(t + d, 4))
        send(*hop(1, block, 0, n, "sp", across))
        send(*hop(2, block, 0, n, "sp", twin))
    for n in range(NCH):
        for d in (1, 3, 2):
            block = fin.at[s, lax.rem(t - d + 4, 4), :, cols[n]]
            arrived(*hop(0, block, d, n, "tp", lax.rem(t + d, 4)))
            send(*hop(1, block, d, n, "sp", across))
            send(*hop(2, block, d, n, "sp", twin))
    for n in range(NCH):
        for d in range(4):
            block = fin.at[across, lax.rem(t - d + 4, 4), :, cols[n]]
            arrived(*hop(1, block, d, n, "sp", across))
            send(*hop(3, block, d, n, "sp", twin))
    gathered(1, kv1)
    for i in range(4):
        kv1_out[i * ROWS:(i + 1) * ROWS, :] = kv1[i]
    for n in range(NCH):
        for d in range(4):
            arrived(*hop(2, fin.at[twin, lax.rem(t - d + 4, 4), :, cols[n]], d, n, "sp", twin))
            arrived(*hop(3, fin.at[diagonal, lax.rem(t - d + 4, 4), :, cols[n]], d, n, "sp", twin))
    for i in range(4):
        hid[i * ROWS:(i + 1) * ROWS, :] = jnp.concatenate([fin[i, j] for j in range(4)], axis=0).astype(BF16)
    for key in list(unsent):
        flush(key)


def solution(mesh):
    cache_spec = P(None, "dp", "sp", "tp", None)
    in_specs = (P("dp", None), P("dp"), cache_spec, cache_spec, P(), P(), P(None, None, "tp"), P(None, "tp"),
                P(None, "tp", None), P(), P(None, None, "tp"), P(None, "tp"), P(None, "tp", None), P())
    out_specs = (P("dp", None), cache_spec, cache_spec)
    table = rope_table()
    vmem, hbm = (pl.BlockSpec(memory_space=m) for m in (pltpu.VMEM, pl.ANY))
    dma = pltpu.SemaphoreType.DMA

    def device_step(hidden, positions, k_cache, v_cache, ln_gain, ln_bias, w_qkv, b_qkv, w_dense, b_dense,
                    w_up, b_up, w_down, b_down):
        flat = (2, SEQS, SLOTS * KV, HEAD)
        kc, vc = k_cache.reshape(flat), v_cache.reshape(flat)
        cache = jax.ShapeDtypeStruct(flat, BF16)
        row8 = [pltpu.VMEM((SEQS * 8, n * HEAD), F32) for n in (1, 2, 1, 1)]
        buffers = [pltpu.VMEM(flat[1:], BF16)] * 2
        rows = [jax.ShapeDtypeStruct((SEQS, n), F32) for n in (QW, KVW, STAT, HEAD, HEAD)]
        big = pltpu.CompilerParams(vmem_limit_bytes=VMEM_MAX)
        ko, vo, q0, kv0, stats0, cos_rows, sin_rows = pl.pallas_call(
            entry_kernel,
            out_shape=(cache, cache, *rows),
            in_specs=[hbm] * 9,
            out_specs=(hbm,) * 7,
            scratch_shapes=[pltpu.SMEM((SEQS,), jnp.int32), pltpu.VMEM((SEQS, D), BF16), pltpu.VMEM((2, 2, D), BF16),
                            pltpu.VMEM((2, 2, D), BF16), pltpu.VMEM((2, QKV), BF16), pltpu.VMEM((SEQ_LEN, HEAD), F32)]
            + [pltpu.VMEM(x.shape, F32) for x in rows] + [pltpu.VMEM((D, QKV), BF16)] + buffers
            + [pltpu.VMEM((SEQS, D), BF16), pltpu.VMEM((SEQS, QKV), F32)] + row8 + [dma((NCH,)), dma((4, NGRP)), dma((6,))],
            compiler_params=big,
            name="entry",
        )(positions, hidden, ln_gain, ln_bias, b_qkv, table, w_qkv, kc, vc)

        hid, kv1 = pl.pallas_call(
            main_kernel,
            out_shape=(jax.ShapeDtypeStruct((SEQS, D), BF16), rows[1]),
            in_specs=[hbm] * 19,
            out_specs=(vmem, vmem),
            scratch_shapes=[
                pltpu.SMEM((SEQS,), jnp.int32), pltpu.VMEM((ROWS, QW), F32), pltpu.VMEM((ROWS, KVW), F32),
                pltpu.VMEM((SEQS, STAT), F32), pltpu.VMEM((ROWS, HEAD), F32), pltpu.VMEM((ROWS, HEAD), F32),
                pltpu.VMEM((ROWS, D), BF16), pltpu.VMEM((2, 2, D), BF16), pltpu.VMEM((2, 2, D), BF16),
                pltpu.VMEM((2, QKV), BF16), pltpu.VMEM((2, D), BF16), pltpu.VMEM((2, UP), BF16),
                pltpu.VMEM((2, D), BF16), dma((13,)),
                pltpu.VMEM((D, QKV), BF16), pltpu.VMEM((QW, D), BF16), pltpu.VMEM((D, UP), BF16),
                pltpu.VMEM((FF, D), BF16)] + buffers + [
                pltpu.VMEM((2, 3, ROWS, STAT), F32),
                pltpu.VMEM((2, 4, OWN, D), F32),
                pltpu.VMEM((2, 3, OWN, D), F32),
                pltpu.VMEM((2, 4, OWN, D), F32),
                pltpu.VMEM((OWN, D), F32),
                pltpu.VMEM((ROWS, QW), BF16),
                pltpu.VMEM((ROWS, CH), BF16),
                pltpu.VMEM((ROWS, UP), F32),
                pltpu.VMEM((ROWS, FF), BF16),
                pltpu.VMEM((ROWS, QKV), F32),
                pltpu.VMEM((4, ROWS, QW), F32),
                pltpu.VMEM((4, ROWS, KVW), F32),
                pltpu.VMEM((SEQS, STAT), F32),
                pltpu.VMEM((4, 4, OWN, D), F32),
            ] + row8 + [
                dma((4, NCH)), dma((2,)), dma((2, 3)), dma((2, 3)), dma((4, 3, NCH)), dma((4, 3, NCH)),
                dma((3, 3, NCH)), dma((3, 3, NCH)), dma((2, 3)), dma((2, 3)), dma((4, 4, NCH)), dma((4, 4, NCH)),
                dma((3, NCH))],
            compiler_params=pltpu.CompilerParams(vmem_limit_bytes=VMEM_MAX, collective_id=0, has_side_effects=True),
            name="main",
        )(positions, q0, kv0, stats0, cos_rows, sin_rows, hidden, ln_gain, ln_bias, b_qkv, b_dense, b_up, b_down,
          w_qkv, w_dense, w_up, w_down, kc, vc)

        hidden_out, ko, vo = pl.pallas_call(
            exit_kernel,
            out_shape=(jax.ShapeDtypeStruct((SEQS, D), BF16), cache, cache),
            in_specs=[hbm] * 7,
            out_specs=(hbm, hbm, hbm),
            scratch_shapes=buffers + [pltpu.VMEM((SEQS, KVW), F32), pltpu.VMEM((SEQS, D), BF16),
                                      pltpu.SMEM((SEQS,), jnp.int32), dma((4, NGRP)), dma((4,))],
            input_output_aliases={5: 1, 6: 2},
            compiler_params=big,
            name="exit",
        )(positions, kv1, hid, kc, vc, ko, vo)
        return hidden_out, ko.reshape(k_cache.shape), vo.reshape(v_cache.shape)

    return jax.shard_map(device_step, mesh=mesh, in_specs=in_specs, out_specs=out_specs, check_vma=False)
```
